128 devices in a mesh: dp: 1, tp: 16 (over z, y), cp: 8 (over x, core).
Axes of the slice: x: 4, y: 4, z: 4, core: 2. Of those that a mesh axis runs over, the one named last changes fastest.
Arguments:
- x: bfloat16 [16384, 4608], P(('dp', 'cp', 'tp'))
- w_q: bfloat16 [4608, 4096], P(None, 'tp')
- w_k: bfloat16 [4608, 2048], P(None, 'tp')
- w_v: bfloat16 [4608, 2048], P(None, 'tp')
- w_o: bfloat16 [4096, 4608], P('tp')
Outputs:
- output: bfloat16 [16384, 4608], P(('dp', 'cp', 'tp'))
All inputs are finite; a program needn't handle non-finite values.
Results may differ from the reference program's by a relative error of at most 0.00601587.
Values are sent between devices in bfloat16 or wider.
A program may use at most 1 GiB of HBM per device.

```python
import jax
import jax.numpy as jnp
from jax import lax

D = 4608
HEADS = 32
KV_HEADS = 16
HEAD = 128
SEQ = 16384
CP = 8
Q_BLOCK = 128


def stored_positions():
    piece_len = SEQ // (2 * CP)
    row_idx = jnp.arange(SEQ)
    block_idx = row_idx // (2 * piece_len)
    within = row_idx % (2 * piece_len)
    return jnp.where(within < piece_len, block_idx * piece_len + within, (2 * CP - 1 - block_idx) * piece_len + within - piece_len)


def setup_inputs(seed: int = 0, part: int = 0) -> dict:
    base_key = jax.random.key(seed)
    key_x = jax.random.fold_in(jax.random.fold_in(base_key, 1), part)
    key_q, key_k, key_v, key_o = jax.random.split(jax.random.fold_in(base_key, 2), 4)
    x_val = jax.random.normal(key_x, (SEQ, D), jnp.float32)
    w_q = jax.random.normal(key_q, (D, HEADS * HEAD), jnp.float32) * (1.6 * D ** -0.5)
    w_k = jax.random.normal(key_k, (D, KV_HEADS * HEAD), jnp.float32) * (1.6 * D ** -0.5)
    w_v = jax.random.normal(key_v, (D, KV_HEADS * HEAD), jnp.float32) * (D ** -0.5)
    w_o = jax.random.normal(key_o, (HEADS * HEAD, D), jnp.float32) * (3.0 * (HEADS * HEAD) ** -0.5)
    return {"x": x_val.astype(jnp.bfloat16), "w_q": w_q.astype(jnp.bfloat16), "w_k": w_k.astype(jnp.bfloat16), "w_v": w_v.astype(jnp.bfloat16), "w_o": w_o.astype(jnp.bfloat16)}


def reference(x, w_q, w_k, w_v, w_o):
    group_size = HEADS // KV_HEADS
    score_scale = HEAD ** -0.5
    q_proj = jnp.dot(x, w_q, preferred_element_type=jnp.float32).astype(jnp.bfloat16)
    k_proj = jnp.dot(x, w_k, preferred_element_type=jnp.float32).astype(jnp.bfloat16)
    v_proj = jnp.dot(x, w_v, preferred_element_type=jnp.float32).astype(jnp.bfloat16)
    q_blocks = q_proj.astype(jnp.float32).reshape(SEQ // Q_BLOCK, Q_BLOCK, KV_HEADS, group_size, HEAD)
    k_heads = jnp.transpose(k_proj.astype(jnp.float32).reshape(SEQ, KV_HEADS, HEAD), (1, 0, 2))
    v_heads = jnp.transpose(v_proj.astype(jnp.float32).reshape(SEQ, KV_HEADS, HEAD), (1, 0, 2))
    positions = stored_positions()
    pos_blocks = positions.reshape(SEQ // Q_BLOCK, Q_BLOCK)

    def one_block(block_args):
        q_blk, pos_blk = block_args
        visible = pos_blk[:, None] >= positions[None, :]

        def one_head(head_args):
            q_head, k_head, v_head = head_args
            scores = jnp.einsum("qge,ke->gqk", q_head, k_head) * score_scale
            scores = jnp.where(visible[None], scores, -jnp.inf)
            row_max = scores.max(axis=-1, keepdims=True)
            p_block = jnp.exp(scores - row_max)
            row_sum = p_block.sum(axis=-1)
            weighted = jnp.einsum("gqk,ke->qge", p_block.astype(jnp.bfloat16).astype(jnp.float32), v_head)
            return weighted / jnp.transpose(row_sum)[:, :, None]

        head_outs = lax.map(one_head, (jnp.transpose(q_blk, (1, 0, 2, 3)), k_heads, v_heads))
        return jnp.transpose(head_outs, (1, 0, 2, 3))

    attn_out = lax.map(one_block, (q_blocks, pos_blocks))
    attn_out = attn_out.reshape(SEQ, HEADS * HEAD).astype(jnp.bfloat16)
    return jnp.dot(attn_out, w_o, preferred_element_type=jnp.float32).astype(jnp.bfloat16)
```

```python
import functools

import jax
import jax.numpy as jnp
from jax import lax
from jax.experimental import pallas as pl
from jax.experimental.pallas import tpu as pltpu
from jax.sharding import PartitionSpec as P

HEAD_DIM = 128
LOG2E = 1.4426950408889634
NT = (((1,), (1,)), ((), ()))
SUB = 512


def attention_kernel(cp_size, q_ref, kv_ref, o_ref, acc_ref, m_ref, l_ref):
    rank = lax.axis_index("cp")
    piece = q_ref.shape[0] // 2
    coef = LOG2E * HEAD_DIM ** -0.5
    group = q_ref.shape[1] // HEAD_DIM
    nsub = piece // SUB
    subs = [(g, s) for g in range(group) for s in range(nsub)]

    def lane_sum(p):
        total = p[:, 0:128]
        for c in range(1, p.shape[1] // 128):
            total = total + p[:, c * 128:(c + 1) * 128]
        return total

    def scores(half, g, s, base, width):
        qs = q_ref[pl.ds(pl.multiple_of(half * piece + s * SUB, SUB), SUB), g * HEAD_DIM:(g + 1) * HEAD_DIM]
        ks = kv_ref[pl.ds(pl.multiple_of(base, SUB), width), 0:HEAD_DIM]
        return lax.dot_general(qs, ks, NT, preferred_element_type=jnp.float32)

    def values(p, base, width):
        vs = kv_ref[pl.ds(pl.multiple_of(base, SUB), width), HEAD_DIM:2 * HEAD_DIM]
        return jnp.dot(p.astype(jnp.bfloat16), vs, preferred_element_type=jnp.float32)

    def diag(half, _):
        base = rank * 2 * piece + half * piece
        for g, s in subs:
            width = (s + 1) * SUB
            sc = scores(half, g, s, base, width)
            row = lax.broadcasted_iota(jnp.int32, (SUB, width), 0) + s * SUB
            col = lax.broadcasted_iota(jnp.int32, (SUB, width), 1)
            sc = jnp.where(row >= col, sc, -jnp.inf)
            top = jnp.max(sc, axis=1, keepdims=True) * coef
            p = jnp.exp2(sc * coef - top)
            slot = pl.ds(pl.multiple_of(half * piece + s * SUB, SUB), SUB)
            m_ref[g, slot, :] = jnp.broadcast_to(top, (SUB, 128))
            l_ref[g, slot, :] = lane_sum(p)
            acc_ref[g, slot, :] = values(p, base, width)
        return 0

    def full(job, _):
        n_high = 2 * cp_size - 1 - rank
        is_high = job < n_high
        half = jnp.where(is_high, 1, 0)
        p_idx = jnp.where(is_high, job, job - n_high)
        first = p_idx < cp_size
        base = jnp.where(first, p_idx * 2 * piece, (2 * cp_size - 1 - p_idx) * 2 * piece + piece)
        nxt = scores(half, *subs[0], base, piece)
        for i, (g, s) in enumerate(subs):
            sc = nxt
            if i + 1 < len(subs):
                nxt = scores(half, *subs[i + 1], base, piece)
            slot = pl.ds(pl.multiple_of(half * piece + s * SUB, SUB), SUB)
            m_old = m_ref[g, slot, :]
            top = jnp.max(sc, axis=1, keepdims=True) * coef
            m_new = jnp.maximum(m_old, top)
            scale = jnp.exp2(m_old - m_new)
            p = jnp.exp2(sc * coef - m_new[:, 0:1])
            m_ref[g, slot, :] = m_new
            l_ref[g, slot, :] = l_ref[g, slot, :] * scale + lane_sum(p)
            acc_ref[g, slot, :] = acc_ref[g, slot, :] * scale + values(p, base, piece)
        return 0

    lax.fori_loop(0, 2, diag, 0)
    lax.fori_loop(0, 2 * cp_size - 1, full, 0)

    def finish(i, _):
        slot = pl.ds(pl.multiple_of(i * SUB, SUB), SUB)
        for g in range(group):
            total = jnp.sum(l_ref[g, slot, :], axis=1, keepdims=True)
            o_ref[slot, g * HEAD_DIM:(g + 1) * HEAD_DIM] = (acc_ref[g, slot, :] / total).astype(jnp.bfloat16)
        return 0

    lax.fori_loop(0, 2 * nsub, finish, 0)


def attention(cp_size, q, kv):
    rows, width = q.shape
    group = width // HEAD_DIM
    flops = 4 * rows * group * HEAD_DIM * (kv.shape[0] // 2)
    vmem = pl.BlockSpec(memory_space=pltpu.VMEM)
    return pl.pallas_call(
        functools.partial(attention_kernel, cp_size),
        out_shape=jax.ShapeDtypeStruct(q.shape, jnp.bfloat16),
        in_specs=[vmem, vmem],
        out_specs=vmem,
        scratch_shapes=[pltpu.VMEM((group, rows, 128), jnp.float32) for _ in range(3)],
        compiler_params=pltpu.CompilerParams(vmem_limit_bytes=50 * 1024 * 1024),
        cost_estimate=pl.CostEstimate(flops=flops, bytes_accessed=kv.size * 2 + q.size * 4, transcendentals=flops // 512),
        name="attention",
    )(q, kv)


def solution(mesh):
    cp_size = mesh.shape["cp"]
    tp_size = mesh.shape["tp"]
    row_spec = P(("dp", "cp", "tp"), None)

    def local_layer(x_loc, w_q, w_k, w_v, w_o):
        model_width = x_loc.shape[1]
        cols = model_width // tp_size
        w_kv = jnp.concatenate([w_k, w_v], axis=1)
        w_cols = lax.all_to_all(w_o, "tp", split_axis=1, concat_axis=0, tiled=True)
        x_block = lax.all_gather(x_loc, "tp", axis=0, tiled=True)
        kv_own = jnp.dot(x_block, w_kv, preferred_element_type=jnp.float32).astype(jnp.bfloat16)
        kv_all = lax.all_gather(kv_own, "cp", axis=0, tiled=True)
        q_own = jnp.dot(x_block, w_q, preferred_element_type=jnp.float32).astype(jnp.bfloat16)
        heads = attention(cp_size, q_own, kv_all)
        heads_all = lax.all_gather(heads, "tp", axis=0, tiled=False)
        w_split = w_cols.reshape(tp_size, heads.shape[1], cols)
        y_cols = jnp.einsum("tsh,thd->sd", heads_all, w_split, preferred_element_type=jnp.float32).astype(jnp.bfloat16)
        return lax.all_to_all(y_cols, "tp", split_axis=0, concat_axis=1, tiled=True)

    return jax.shard_map(local_layer, mesh=mesh, in_specs=(row_spec, P(None, "tp"), P(None, "tp"), P(None, "tp"), P("tp", None)), out_specs=row_spec, check_vma=False)
```

```python
import functools

import jax
import jax.numpy as jnp
from jax import lax
from jax.experimental import pallas as pl
from jax.experimental.pallas import tpu as pltpu
from jax.sharding import PartitionSpec as P

HEAD_DIM = 128
LOG2E = 1.4426950408889634
NT = (((1,), (1,)), ((), ()))
SUB = 512


def attention_kernel(cp_size, q_ref, kv_ref, o_ref, acc_ref, m_ref, l_ref):
    rank = lax.axis_index("cp")
    piece = q_ref.shape[0] // 2
    coef = LOG2E * HEAD_DIM ** -0.5
    group = q_ref.shape[1] // HEAD_DIM
    nsub = piece // SUB
    subs = [(g, s) for g in range(group) for s in range(nsub)]

    def lane_sum(p):
        total = p[:, 0:128]
        for c in range(1, p.shape[1] // 128):
            total = total + p[:, c * 128:(c + 1) * 128]
        return total

    def scores(half, g, s, base, width):
        qs = q_ref[pl.ds(pl.multiple_of(half * piece + s * SUB, SUB), SUB), g * HEAD_DIM:(g + 1) * HEAD_DIM]
        ks = kv_ref[pl.ds(pl.multiple_of(base, SUB), width), 0:HEAD_DIM]
        return lax.dot_general(qs, ks, NT, preferred_element_type=jnp.float32)

    def values(p, base, width):
        vs = kv_ref[pl.ds(pl.multiple_of(base, SUB), width), HEAD_DIM:2 * HEAD_DIM]
        return jnp.dot(p.astype(jnp.bfloat16), vs, preferred_element_type=jnp.float32)

    def diag(half, _):
        base = rank * 2 * piece + half * piece
        for g, s in subs:
            width = (s + 1) * SUB
            sc = scores(half, g, s, base, width)
            row = lax.broadcasted_iota(jnp.int32, (SUB, width), 0) + s * SUB
            col = lax.broadcasted_iota(jnp.int32, (SUB, width), 1)
            sc = jnp.where(row >= col, sc, -jnp.inf)
            top = jnp.max(sc, axis=1, keepdims=True) * coef
            p = jnp.exp2(sc * coef - top)
            slot = pl.ds(pl.multiple_of(half * piece + s * SUB, SUB), SUB)
            m_ref[g, slot, :] = jnp.broadcast_to(top, (SUB, 128))
            l_ref[g, slot, :] = lane_sum(p)
            acc_ref[g, slot, :] = values(p, base, width)
        return 0

    def full(job, _):
        n_high = 2 * cp_size - 1 - rank
        is_high = job < n_high
        half = jnp.where(is_high, 1, 0)
        p_idx = jnp.where(is_high, job, job - n_high)
        first = p_idx < cp_size
        base = jnp.where(first, p_idx * 2 * piece, (2 * cp_size - 1 - p_idx) * 2 * piece + piece)
        nxt = scores(half, *subs[0], base, piece)
        for i, (g, s) in enumerate(subs):
            sc = nxt
            if i + 1 < len(subs):
                nxt = scores(half, *subs[i + 1], base, piece)
            slot = pl.ds(pl.multiple_of(half * piece + s * SUB, SUB), SUB)
            m_old = m_ref[g, slot, :]
            top = jnp.max(sc, axis=1, keepdims=True) * coef
            m_new = jnp.maximum(m_old, top)
            scale = jnp.exp2(m_old - m_new)
            p = jnp.exp2(sc * coef - m_new[:, 0:1])
            m_ref[g, slot, :] = m_new
            l_ref[g, slot, :] = l_ref[g, slot, :] * scale + lane_sum(p)
            acc_ref[g, slot, :] = acc_ref[g, slot, :] * scale + values(p, base, piece)
        return 0

    lax.fori_loop(0, 2, diag, 0)
    lax.fori_loop(0, 2 * cp_size - 1, full, 0)

    def finish(i, _):
        slot = pl.ds(pl.multiple_of(i * SUB, SUB), SUB)
        for g in range(group):
            total = jnp.sum(l_ref[g, slot, :], axis=1, keepdims=True)
            o_ref[slot, g * HEAD_DIM:(g + 1) * HEAD_DIM] = (acc_ref[g, slot, :] / total).astype(jnp.bfloat16)
        return 0

    lax.fori_loop(0, 2 * nsub, finish, 0)


def attention(cp_size, q, kv):
    rows, width = q.shape
    group = width // HEAD_DIM
    flops = 4 * rows * group * HEAD_DIM * (kv.shape[0] // 2)
    vmem = pl.BlockSpec(memory_space=pltpu.VMEM)
    return pl.pallas_call(
        functools.partial(attention_kernel, cp_size),
        out_shape=jax.ShapeDtypeStruct(q.shape, jnp.bfloat16),
        in_specs=[vmem, vmem],
        out_specs=vmem,
        scratch_shapes=[pltpu.VMEM((group, rows, 128), jnp.float32) for _ in range(3)],
        compiler_params=pltpu.CompilerParams(vmem_limit_bytes=50 * 1024 * 1024),
        cost_estimate=pl.CostEstimate(flops=flops, bytes_accessed=kv.size * 2 + q.size * 4, transcendentals=flops // 512),
        name="attention",
    )(q, kv)


MESH = pl.DeviceIdType.MESH
X_SUB = 2


def front_kernel(tp_size, cp_size, x_hbm, wq_hbm, wk_hbm, wv_hbm, q_hbm, kv_hbm, xg, w_buf, q_buf, kv, load_sem, ring_send, ring_recv, kv_send, left_recv, right_recv, far_recv, pair_recv):
    tp = lax.axis_index("tp")
    cp = lax.axis_index("cp")
    side = 4
    zi, yi = tp // side, lax.rem(tp, side)
    chip, core = cp // 2, lax.rem(cp, 2)
    n_chip = cp_size // 2
    rows = x_hbm.shape[0]
    block = rows * tp_size
    part = rows // 4
    sub = part // X_SUB
    q_width = wq_hbm.shape[1]
    k_width = wk_hbm.shape[1]
    pos = (zi * side + lax.rem(yi + zi, side), yi * side + lax.rem(zi + yi, side))

    def member(cycle, k):
        k = lax.rem(k + 2 * tp_size, tp_size)
        major = k // side
        minor = lax.rem(k - major + side, side)
        return major * side + minor if cycle == 0 else minor * side + major

    streams = [(0, 1), (0, -1), (1, 1), (1, -1)]
    nxt = [member(c, pos[c] + d) for c, d in streams]
    right = lax.rem(chip + 1, n_chip) * 2 + core
    left = lax.rem(chip + n_chip - 1, n_chip) * 2 + core
    far = lax.rem(chip + 2, n_chip) * 2 + core
    pair = cp + 1 - 2 * core
    ahead = jnp.where(core == 0, right, left)
    behind = jnp.where(core == 0, left, right)

    w_q = pltpu.make_async_copy(wq_hbm, w_buf.at[:, pl.ds(0, q_width)], load_sem.at[0])
    w_k = pltpu.make_async_copy(wk_hbm, w_buf.at[:, pl.ds(q_width, k_width)], load_sem.at[1])
    w_v = pltpu.make_async_copy(wv_hbm, w_buf.at[:, pl.ds(q_width + k_width, k_width)], load_sem.at[2])
    own = pltpu.make_async_copy(x_hbm, xg.at[pl.ds(pl.multiple_of(tp * rows, rows), rows)], load_sem.at[3])
    own.start()
    w_q.start()
    w_k.start()
    w_v.start()

    barrier = pltpu.get_barrier_semaphore()
    for peer in nxt:
        pl.semaphore_signal(barrier, inc=1, device_id={"tp": peer}, device_id_type=MESH)
    for peer in (left, right, pair):
        pl.semaphore_signal(barrier, inc=1, device_id={"cp": peer}, device_id_type=MESH)
    pl.semaphore_wait(barrier, 7)
    own.wait()

    def source(s, t):
        c, d = streams[s]
        return member(c, pos[c] - d * t)

    def ring(s, t, u):
        at = xg.at[pl.ds(pl.multiple_of(source(s, t) * rows + s * part + u * sub, sub), sub)]
        return at, dict(send_sem=ring_send.at[s], device_id={"tp": nxt[s]}, device_id_type=MESH)

    def move(ref, send_sem, recv_sem, axis, peer):
        return pltpu.make_async_remote_copy(src_ref=ref, dst_ref=ref, send_sem=send_sem, recv_sem=recv_sem, device_id={axis: peer}, device_id_type=MESH)

    def kv_rows(owner, s, t):
        return kv.at[pl.ds(pl.multiple_of(owner * block + source(s, t) * rows + s * part, part), part)]

    def kv_wait(sem, count):
        ref = kv.at[pl.ds(0, count)]
        pltpu.make_async_remote_copy(src_ref=ref, dst_ref=ref, send_sem=kv_send.at[0], recv_sem=sem, device_id={"cp": pair}, device_id_type=MESH).wait_recv()

    def step(t, _):
        @pl.when(t < tp_size)
        def _():
            for u in range(X_SUB):
                for s in range(4):
                    at = xg.at[pl.ds(pl.multiple_of(source(s, t) * rows + s * part + u * sub, sub), sub)]

                    @pl.when(t > 0)
                    def _():
                        move(at, ring_send.at[s], ring_recv.at[s, t - 1, u], "tp", nxt[s]).wait_recv()

                    @pl.when(t < tp_size - 1)
                    def _():
                        move(at, ring_send.at[s], ring_recv.at[s, t, u], "tp", nxt[s]).start()

        @pl.when(jnp.logical_and(t >= 1, t <= tp_size))
        def _():
            for s in range(4):
                at = kv_rows(cp, s, t - 1)
                move(at, kv_send.at[0], left_recv.at[t - 1], "cp", right).start()
                move(at, kv_send.at[1], right_recv.at[t - 1], "cp", left).start()
                move(at, kv_send.at[2], pair_recv.at[0], "cp", pair).start()

        @pl.when(jnp.logical_and(t >= 3, t <= tp_size + 2))
        def _():
            kv_wait(left_recv.at[t - 3], rows)
            kv_wait(right_recv.at[t - 3], rows)
            for s in range(4):
                move(kv_rows(behind, s, t - 3), kv_send.at[3], far_recv.at[t - 3], "cp", ahead).start()
                move(kv_rows(left, s, t - 3), kv_send.at[4], pair_recv.at[1], "cp", pair).start()
                move(kv_rows(right, s, t - 3), kv_send.at[5], pair_recv.at[2], "cp", pair).start()

        @pl.when(t >= 5)
        def _():
            kv_wait(far_recv.at[t - 5], rows)
            for s in range(4):
                move(kv_rows(far, s, t - 5), kv_send.at[6], pair_recv.at[3], "cp", pair).start()

        @pl.when(t == 0)
        def _():
            w_q.wait()
            w_k.wait()
            w_v.wait()

        @pl.when(t < tp_size)
        def _():
            offs = [pl.multiple_of(source(s, t) * rows + s * part, part) for s in range(4)]
            lhs = jnp.concatenate([xg[pl.ds(o, part), :] for o in offs], axis=0)
            res = jnp.dot(lhs, w_buf[...], preferred_element_type=jnp.float32).astype(jnp.bfloat16)
            for s in range(4):
                q_buf[pl.ds(offs[s], part), :] = res[s * part:(s + 1) * part, 0:q_width]
                kv[pl.ds(pl.multiple_of(cp * block + offs[s], part), part), :] = res[s * part:(s + 1) * part, q_width:]
        return 0

    lax.fori_loop(0, tp_size + 5, step, 0)

    for k in range(4):
        kv_wait(pair_recv.at[k], block)
    out_q = pltpu.make_async_copy(q_buf, q_hbm, load_sem.at[0])
    out_kv = pltpu.make_async_copy(kv, kv_hbm, load_sem.at[1])
    out_q.start()
    out_kv.start()
    for s in range(4):
        ref = xg.at[pl.ds(0, (tp_size - 1) * part)]
        pltpu.make_async_remote_copy(src_ref=ref, dst_ref=ref, send_sem=ring_send.at[s], recv_sem=ring_recv.at[s, 0, 0], device_id={"tp": nxt[s]}, device_id_type=MESH).wait_send()
    for k in range(7):
        ref = kv.at[pl.ds(0, block)]
        pltpu.make_async_remote_copy(src_ref=ref, dst_ref=ref, send_sem=kv_send.at[k], recv_sem=pair_recv.at[0], device_id={"cp": pair}, device_id_type=MESH).wait_send()
    out_q.wait()
    out_kv.wait()


def front(tp_size, cp_size, x_loc, w_q, w_k, w_v):
    rows, depth = x_loc.shape
    block = rows * tp_size
    q_width = w_q.shape[1]
    kv_width = w_k.shape[1] + w_v.shape[1]
    any_space = pl.BlockSpec(memory_space=pl.ANY)
    dma = pltpu.SemaphoreType.DMA
    return pl.pallas_call(
        functools.partial(front_kernel, tp_size, cp_size),
        out_shape=(jax.ShapeDtypeStruct((block, q_width), jnp.bfloat16), jax.ShapeDtypeStruct((block * cp_size, kv_width), jnp.bfloat16)),
        in_specs=[any_space] * 4,
        out_specs=(any_space, any_space),
        scratch_shapes=[
            pltpu.VMEM((block, depth), jnp.bfloat16),
            pltpu.VMEM((depth, q_width + kv_width), jnp.bfloat16),
            pltpu.VMEM((block, q_width), jnp.bfloat16),
            pltpu.VMEM((block * cp_size, kv_width), jnp.bfloat16),
            dma((4,)), dma((4,)), dma((4, tp_size - 1, X_SUB)), dma((7,)), dma((tp_size,)), dma((tp_size,)), dma((tp_size,)), dma((4,)),
        ],
        compiler_params=pltpu.CompilerParams(collective_id=0, has_side_effects=True, vmem_limit_bytes=56 * 1024 * 1024),
        cost_estimate=pl.CostEstimate(flops=2 * block * depth * (q_width + kv_width), bytes_accessed=block * depth * 2, transcendentals=0),
        name="front",
    )(x_loc, w_q, w_k, w_v)


def solution(mesh):
    cp_size = mesh.shape["cp"]
    tp_size = mesh.shape["tp"]
    row_spec = P(("dp", "cp", "tp"), None)

    def local_layer(x_loc, w_q, w_k, w_v, w_o):
        model_width = x_loc.shape[1]
        cols = model_width // tp_size
        w_cols = lax.all_to_all(w_o, "tp", split_axis=1, concat_axis=0, tiled=True)
        q_own, kv_all = front(tp_size, cp_size, x_loc, w_q, w_k, w_v)
        heads = attention(cp_size, q_own, kv_all)
        heads_all = lax.all_gather(heads, "tp", axis=0, tiled=False)
        w_split = w_cols.reshape(tp_size, heads.shape[1], cols)
        y_cols = jnp.einsum("tsh,thd->sd", heads_all, w_split, preferred_element_type=jnp.float32).astype(jnp.bfloat16)
        return lax.all_to_all(y_cols, "tp", split_axis=0, concat_axis=1, tiled=True)

    return jax.shard_map(local_layer, mesh=mesh, in_specs=(row_spec, P(None, "tp"), P(None, "tp"), P(None, "tp"), P("tp", None)), out_specs=row_spec, check_vma=False)
```

```python
import functools

import jax
import jax.numpy as jnp
from jax import lax
from jax.experimental import pallas as pl
from jax.experimental.pallas import tpu as pltpu
from jax.sharding import PartitionSpec as P

HEAD_DIM = 128
LOG2E = 1.4426950408889634
NT = (((1,), (1,)), ((), ()))
SUB = 512


MESH = pl.DeviceIdType.MESH
X_SUB = 2


def front_kernel(tp_size, cp_size, x_hbm, wq_hbm, wk_hbm, wv_hbm, q_hbm, kv_hbm, xg, w_buf, q_buf, kv, load_sem, ring_send, ring_recv, kv_send, left_recv, right_recv, far_recv, pair_recv):
    tp = lax.axis_index("tp")
    cp = lax.axis_index("cp")
    side = 4
    zi, yi = tp // side, lax.rem(tp, side)
    chip, core = cp // 2, lax.rem(cp, 2)
    n_chip = cp_size // 2
    rows = x_hbm.shape[0]
    block = rows * tp_size
    part = rows // 4
    sub = part // X_SUB
    q_width = wq_hbm.shape[1]
    k_width = wk_hbm.shape[1]
    pos = (zi * side + lax.rem(yi + zi, side), yi * side + lax.rem(zi + yi, side))

    def member(cycle, k):
        k = lax.rem(k + 2 * tp_size, tp_size)
        major = k // side
        minor = lax.rem(k - major + side, side)
        return major * side + minor if cycle == 0 else minor * side + major

    streams = [(0, 1), (0, -1), (1, 1), (1, -1)]
    nxt = [member(c, pos[c] + d) for c, d in streams]
    right = lax.rem(chip + 1, n_chip) * 2 + core
    left = lax.rem(chip + n_chip - 1, n_chip) * 2 + core
    far = lax.rem(chip + 2, n_chip) * 2 + core
    pair = cp + 1 - 2 * core
    ahead = jnp.where(core == 0, right, left)
    behind = jnp.where(core == 0, left, right)

    w_q = pltpu.make_async_copy(wq_hbm, w_buf.at[:, pl.ds(0, q_width)], load_sem.at[0])
    w_k = pltpu.make_async_copy(wk_hbm, w_buf.at[:, pl.ds(q_width, k_width)], load_sem.at[1])
    w_v = pltpu.make_async_copy(wv_hbm, w_buf.at[:, pl.ds(q_width + k_width, k_width)], load_sem.at[2])
    own = pltpu.make_async_copy(x_hbm, xg.at[pl.ds(pl.multiple_of(tp * rows, rows), rows)], load_sem.at[3])
    own.start()
    w_q.start()
    w_k.start()
    w_v.start()

    barrier = pltpu.get_barrier_semaphore()
    for peer in nxt:
        pl.semaphore_signal(barrier, inc=1, device_id={"tp": peer}, device_id_type=MESH)
    for peer in (left, right, pair):
        pl.semaphore_signal(barrier, inc=1, device_id={"cp": peer}, device_id_type=MESH)
    pl.semaphore_wait(barrier, 7)
    own.wait()

    def source(s, t):
        c, d = streams[s]
        return member(c, pos[c] - d * t)

    def ring(s, t, u):
        at = xg.at[pl.ds(pl.multiple_of(source(s, t) * rows + s * part + u * sub, sub), sub)]
        return at, dict(send_sem=ring_send.at[s], device_id={"tp": nxt[s]}, device_id_type=MESH)

    def move(ref, send_sem, recv_sem, axis, peer):
        return pltpu.make_async_remote_copy(src_ref=ref, dst_ref=ref, send_sem=send_sem, recv_sem=recv_sem, device_id={axis: peer}, device_id_type=MESH)

    def kv_rows(owner, s, t):
        return kv.at[pl.ds(pl.multiple_of(owner * block + source(s, t) * rows + s * part, part), part)]

    def kv_wait(sem, count):
        ref = kv.at[pl.ds(0, count)]
        pltpu.make_async_remote_copy(src_ref=ref, dst_ref=ref, send_sem=kv_send.at[0], recv_sem=sem, device_id={"cp": pair}, device_id_type=MESH).wait_recv()

    def step(t, _):
        @pl.when(t < tp_size)
        def _():
            for u in range(X_SUB):
                for s in range(4):
                    at = xg.at[pl.ds(pl.multiple_of(source(s, t) * rows + s * part + u * sub, sub), sub)]

                    @pl.when(t > 0)
                    def _():
                        move(at, ring_send.at[s], ring_recv.at[s, t - 1, u], "tp", nxt[s]).wait_recv()

                    @pl.when(t < tp_size - 1)
                    def _():
                        move(at, ring_send.at[s], ring_recv.at[s, t, u], "tp", nxt[s]).start()

        @pl.when(jnp.logical_and(t >= 1, t <= tp_size))
        def _():
            for s in range(4):
                at = kv_rows(cp, s, t - 1)
                move(at, kv_send.at[0], left_recv.at[t - 1], "cp", right).start()
                move(at, kv_send.at[1], right_recv.at[t - 1], "cp", left).start()
                move(at, kv_send.at[2], pair_recv.at[0], "cp", pair).start()

        @pl.when(jnp.logical_and(t >= 3, t <= tp_size + 2))
        def _():
            kv_wait(left_recv.at[t - 3], rows)
            kv_wait(right_recv.at[t - 3], rows)
            for s in range(4):
                move(kv_rows(behind, s, t - 3), kv_send.at[3], far_recv.at[t - 3], "cp", ahead).start()
                move(kv_rows(left, s, t - 3), kv_send.at[4], pair_recv.at[1], "cp", pair).start()
                move(kv_rows(right, s, t - 3), kv_send.at[5], pair_recv.at[2], "cp", pair).start()

        @pl.when(t >= 5)
        def _():
            kv_wait(far_recv.at[t - 5], rows)
            for s in range(4):
                move(kv_rows(far, s, t - 5), kv_send.at[6], pair_recv.at[3], "cp", pair).start()

        @pl.when(t == 0)
        def _():
            w_q.wait()
            w_k.wait()
            w_v.wait()

        @pl.when(t < tp_size)
        def _():
            offs = [pl.multiple_of(source(s, t) * rows + s * part, part) for s in range(4)]
            lhs = jnp.concatenate([xg[pl.ds(o, part), :] for o in offs], axis=0)
            res = jnp.dot(lhs, w_buf[...], preferred_element_type=jnp.float32).astype(jnp.bfloat16)
            for s in range(4):
                q_buf[pl.ds(offs[s], part), :] = res[s * part:(s + 1) * part, 0:q_width]
                kv[pl.ds(pl.multiple_of(cp * block + offs[s], part), part), :] = res[s * part:(s + 1) * part, q_width:]
        return 0

    lax.fori_loop(0, tp_size + 5, step, 0)

    for k in range(4):
        kv_wait(pair_recv.at[k], block)
    out_q = pltpu.make_async_copy(q_buf, q_hbm, load_sem.at[0])
    out_kv = pltpu.make_async_copy(kv, kv_hbm, load_sem.at[1])
    out_q.start()
    out_kv.start()
    for s in range(4):
        ref = xg.at[pl.ds(0, (tp_size - 1) * part)]
        pltpu.make_async_remote_copy(src_ref=ref, dst_ref=ref, send_sem=ring_send.at[s], recv_sem=ring_recv.at[s, 0, 0], device_id={"tp": nxt[s]}, device_id_type=MESH).wait_send()
    for k in range(7):
        ref = kv.at[pl.ds(0, block)]
        pltpu.make_async_remote_copy(src_ref=ref, dst_ref=ref, send_sem=kv_send.at[k], recv_sem=pair_recv.at[0], device_id={"cp": pair}, device_id_type=MESH).wait_send()
    out_q.wait()
    out_kv.wait()


def front(tp_size, cp_size, x_loc, w_q, w_k, w_v):
    rows, depth = x_loc.shape
    block = rows * tp_size
    q_width = w_q.shape[1]
    kv_width = w_k.shape[1] + w_v.shape[1]
    any_space = pl.BlockSpec(memory_space=pl.ANY)
    dma = pltpu.SemaphoreType.DMA
    return pl.pallas_call(
        functools.partial(front_kernel, tp_size, cp_size),
        out_shape=(jax.ShapeDtypeStruct((block, q_width), jnp.bfloat16), jax.ShapeDtypeStruct((block * cp_size, kv_width), jnp.bfloat16)),
        in_specs=[any_space] * 4,
        out_specs=(any_space, any_space),
        scratch_shapes=[
            pltpu.VMEM((block, depth), jnp.bfloat16),
            pltpu.VMEM((depth, q_width + kv_width), jnp.bfloat16),
            pltpu.VMEM((block, q_width), jnp.bfloat16),
            pltpu.VMEM((block * cp_size, kv_width), jnp.bfloat16),
            dma((4,)), dma((4,)), dma((4, tp_size - 1, X_SUB)), dma((7,)), dma((tp_size,)), dma((tp_size,)), dma((tp_size,)), dma((4,)),
        ],
        compiler_params=pltpu.CompilerParams(collective_id=0, has_side_effects=True, vmem_limit_bytes=56 * 1024 * 1024),
        cost_estimate=pl.CostEstimate(flops=2 * block * depth * (q_width + kv_width), bytes_accessed=block * depth * 2, transcendentals=0),
        name="front",
    )(x_loc, w_q, w_k, w_v)


def back_kernel(tp_size, cp_size, q_hbm, kv_hbm, wo_hbm, y_hbm, q_ref, kv_ref, w_buf, wo_buf, og, o_buf, y_send, y_all, acc_ref, m_ref, l_ref, load_sem, w_send, w_recv, d1_send, d1_recv, d2_send, d2_recv, d3_send, d3_recv):
    side = 4
    tp = lax.axis_index("tp")
    rank = lax.axis_index("cp")
    zi, yi = tp // side, lax.rem(tp, side)
    chip, core = rank // 2, lax.rem(rank, 2)
    n_chip = cp_size // 2
    piece = q_ref.shape[0] // 2
    group = q_ref.shape[1] // HEAD_DIM
    chunk = SUB // side
    slab = wo_buf.shape[0]
    head_rows = slab * cp_size
    cols = w_buf.shape[1]
    coef = LOG2E * HEAD_DIM ** -0.5
    right = lax.rem(chip + 1, n_chip) * 2 + core
    left = lax.rem(chip + n_chip - 1, n_chip) * 2 + core
    far = lax.rem(chip + 2, n_chip) * 2 + core
    pair = rank + 1 - 2 * core
    ahead = jnp.where(core == 0, right, left)
    behind = jnp.where(core == 0, left, right)
    up = lax.rem(zi + 1, side)
    down = lax.rem(zi + side - 1, side)
    z_far = lax.rem(zi + 2, side)

    load_q = pltpu.make_async_copy(q_hbm, q_ref, load_sem.at[0])
    load_kv = pltpu.make_async_copy(kv_hbm, kv_ref, load_sem.at[1])
    load_w = pltpu.make_async_copy(wo_hbm.at[pl.ds(pl.multiple_of(rank * slab, slab), slab)], wo_buf, load_sem.at[2])
    load_w.start()
    load_q.start()
    load_kv.start()
    barrier = pltpu.get_barrier_semaphore()
    for k in range(1, tp_size):
        pl.semaphore_signal(barrier, inc=1, device_id={"tp": lax.rem(tp + k, tp_size)}, device_id_type=MESH)
    for peer in (left, right, pair):
        pl.semaphore_signal(barrier, inc=1, device_id={"cp": peer}, device_id_type=MESH)
    pl.semaphore_wait(barrier, tp_size + 2)

    def move(src, dst, send_sem, recv_sem, axis, peer):
        return pltpu.make_async_remote_copy(src_ref=src, dst_ref=dst, send_sem=send_sem, recv_sem=recv_sem, device_id={axis: peer}, device_id_type=MESH)

    def got(ref, recv_sem):
        move(ref, ref, w_send.at[0], recv_sem, "cp", pair).wait_recv()

    def sent(ref, send_sem):
        move(ref, ref, send_sem, w_recv.at[0], "cp", pair).wait_send()

    def w_rows(owner, member):
        return w_buf.at[pl.ds(pl.multiple_of(owner * head_rows + member * slab, slab), slab)]

    def w_cols(quarter):
        return wo_buf.at[:, pl.ds(pl.multiple_of(quarter * cols, 128), cols)]

    load_w.wait()
    own_w = pltpu.make_async_copy(w_cols(zi), w_rows(tp, rank), load_sem.at[2])
    own_w.start()

    def spread(k, _):
        peer = lax.rem(tp + k, tp_size)
        move(w_cols(peer // side), w_rows(tp, rank), w_send.at[0], w_recv.at[0], "tp", peer).start()
        return 0

    lax.fori_loop(1, tp_size, spread, 0)

    def w_share():
        own_w.wait()
        got(w_buf.at[pl.ds(0, (tp_size - 1) * slab)], w_recv.at[0])

        def one(s, _):
            ref = w_rows(s, rank)
            move(ref, ref, w_send.at[1], w_recv.at[1], "cp", right).start()
            move(ref, ref, w_send.at[2], w_recv.at[2], "cp", left).start()
            move(ref, ref, w_send.at[3], w_recv.at[4], "cp", pair).start()
            return 0

        lax.fori_loop(0, tp_size, one, 0)

    w_part = w_buf.at[pl.ds(0, tp_size * slab)]

    def w_pass():
        got(w_part, w_recv.at[1])
        got(w_part, w_recv.at[2])

        def one(s, _):
            ref = w_rows(s, behind)
            move(ref, ref, w_send.at[4], w_recv.at[3], "cp", ahead).start()
            ref = w_rows(s, left)
            move(ref, ref, w_send.at[5], w_recv.at[5], "cp", pair).start()
            ref = w_rows(s, right)
            move(ref, ref, w_send.at[6], w_recv.at[6], "cp", pair).start()
            return 0

        lax.fori_loop(0, tp_size, one, 0)

    def w_last():
        got(w_part, w_recv.at[3])

        def one(s, _):
            ref = w_rows(s, far)
            move(ref, ref, w_send.at[7], w_recv.at[7], "cp", pair).start()
            return 0

        lax.fori_loop(0, tp_size, one, 0)

    def lane_sum(p):
        total = p[:, 0:128]
        for c in range(1, p.shape[1] // 128):
            total = total + p[:, c * 128:(c + 1) * 128]
        return total

    def scores(i, g, base, width):
        qs = q_ref[pl.ds(pl.multiple_of(i * SUB, SUB), SUB), g * HEAD_DIM:(g + 1) * HEAD_DIM]
        ks = kv_ref[pl.ds(pl.multiple_of(base, SUB), width), 0:HEAD_DIM]
        return lax.dot_general(qs, ks, NT, preferred_element_type=jnp.float32)

    def values(p, base, width):
        vs = kv_ref[pl.ds(pl.multiple_of(base, SUB), width), HEAD_DIM:2 * HEAD_DIM]
        return jnp.dot(p.astype(jnp.bfloat16), vs, preferred_element_type=jnp.float32)

    def diag(i, s):
        width = (s + 1) * SUB
        base = rank * 2 * piece + (i // 2) * piece
        for g in range(group):
            sc = scores(i, g, base, width)
            row = lax.broadcasted_iota(jnp.int32, (SUB, width), 0) + s * SUB
            col = lax.broadcasted_iota(jnp.int32, (SUB, width), 1)
            sc = jnp.where(row >= col, sc, -jnp.inf)
            top = jnp.max(sc, axis=1, keepdims=True) * coef
            p = jnp.exp2(sc * coef - top)
            m_ref[g] = jnp.broadcast_to(top, (SUB, 128))
            l_ref[g] = lane_sum(p)
            acc_ref[g] = values(p, base, width)

    def d1(i, k):
        peer = lax.rem(yi + k, side)
        return move(o_buf.at[i, peer], og.at[i, tp], d1_send.at[0], d1_recv.at[i], "tp", zi * side + peer)

    def tile_part(i, z, half):
        return og.at[i, pl.ds(z * side, side), pl.ds(half * (chunk // 2), chunk // 2)]

    def d2(i, z, half, send, recv, peer):
        ref = tile_part(i, z, half)
        return move(ref, ref, d2_send.at[send], d2_recv.at[i, recv], "tp", peer * side + yi)

    def gather_start(i):
        got(og.at[i, pl.ds(0, side - 1)], d1_recv.at[i])
        d2(i, zi, 0, 0, 0, up).start()
        d2(i, zi, 1, 1, 2, down).start()
        d2(i, zi, 1, 0, 1, up).start()
        d2(i, zi, 0, 1, 3, down).start()

    def gather_pass(i):
        got(tile_part(i, down, 0), d2_recv.at[i, 0])
        d2(i, down, 0, 2, 4, up).start()
        got(tile_part(i, up, 1), d2_recv.at[i, 2])
        d2(i, up, 1, 3, 5, down).start()

    def gather_end(i):
        got(tile_part(i, down, 1), d2_recv.at[i, 1])
        got(tile_part(i, up, 0), d2_recv.at[i, 3])
        got(tile_part(i, z_far, 0), d2_recv.at[i, 4])
        got(tile_part(i, z_far, 1), d2_recv.at[i, 5])

    y_mine = y_all.at[:, pl.ds(pl.multiple_of(zi * cols, 128), cols)]

    def project(i):
        lhs = jnp.concatenate([og[i, s] for s in range(tp_size)], axis=1)
        y_send[i] = jnp.dot(lhs, w_buf[...], preferred_element_type=jnp.float32).astype(jnp.bfloat16)

    def deliver(i):
        @pl.when(zi != i)
        def _():
            move(y_send.at[i], y_mine, d3_send.at[0], d3_recv.at[0], "tp", i * side + yi).start()

        @pl.when(zi == i)
        def _():
            y_all[:, pl.ds(pl.multiple_of(zi * cols, 128), cols)] = y_send[i]

    load_q.wait()
    load_kv.wait()

    def tile(i, _):
        is_low = i < 2
        count = jnp.where(is_low, rank, 2 * cp_size - 1 - rank)
        before = jnp.where(is_low, i * rank, 2 * rank + (i - 2) * (2 * cp_size - 1 - rank))

        @pl.when(lax.rem(i, 2) == 0)
        def _():
            diag(i, 0)

        @pl.when(lax.rem(i, 2) == 1)
        def _():
            diag(i, 1)

        @pl.when(i == 2)
        def _():
            gather_start(0)
            gather_start(1)

        @pl.when(i == 3)
        def _():
            gather_start(2)

        def full(j, _):
            first = j < cp_size
            base = jnp.where(first, j * 2 * piece, (2 * cp_size - 1 - j) * 2 * piece + piece)
            turn = before + j
            pl.when(turn == 10)(w_share)
            pl.when(turn == 22)(w_pass)
            pl.when(turn == 28)(w_last)
            nxt = scores(i, 0, base, piece)
            for g in range(group):
                sc = nxt
                if g + 1 < group:
                    nxt = scores(i, g + 1, base, piece)
                m_old = m_ref[g]
                top = jnp.max(sc, axis=1, keepdims=True) * coef
                m_new = jnp.maximum(m_old, top)
                scale = jnp.exp2(m_old - m_new)
                p = jnp.exp2(sc * coef - m_new[:, 0:1])
                m_ref[g] = m_new
                l_ref[g] = l_ref[g] * scale + lane_sum(p)
                acc_ref[g] = acc_ref[g] * scale + values(p, base, piece)
            return 0

        early = jnp.minimum(count, 6)
        lax.fori_loop(0, early, full, 0)

        @pl.when(i == 2)
        def _():
            gather_pass(0)
            gather_pass(1)

        @pl.when(i == 3)
        def _():
            gather_pass(2)

        lax.fori_loop(early, count, full, 0)
        for g in range(group):
            total = jnp.sum(l_ref[g], axis=1, keepdims=True)
            out = (acc_ref[g] / total).astype(jnp.bfloat16)
            for k in range(side):
                o_buf[i, k, :, g * HEAD_DIM:(g + 1) * HEAD_DIM] = out[k * chunk:(k + 1) * chunk]
        og[i, tp] = o_buf[i, yi]
        for k in range(1, side):
            d1(i, k).start()
        return 0

    lax.fori_loop(0, side, tile, 0)

    gather_start(3)
    for k in range(4, 8):
        got(w_part, w_recv.at[k])
    for i in range(3):
        gather_end(i)
    lax.fori_loop(0, 3, lambda i, c: (project(i), c)[1], 0)
    gather_pass(3)
    for i in range(3):
        deliver(i)
    gather_end(3)
    project(3)
    deliver(3)
    got(y_all.at[:, pl.ds(0, 3 * cols)], d3_recv.at[0])
    out = pltpu.make_async_copy(y_all, y_hbm, load_sem.at[0])
    out.start()
    sent(w_buf.at[pl.ds(0, (tp_size - 1) * slab)], w_send.at[0])
    for k in range(1, 8):
        sent(w_part, w_send.at[k])
    sent(o_buf.at[:, pl.ds(0, side - 1)], d1_send.at[0])
    sent(og.at[:, pl.ds(0, side)], d2_send.at[0])
    sent(og.at[:, pl.ds(0, side)], d2_send.at[1])
    sent(og.at[:, pl.ds(0, side), pl.ds(0, chunk // 2)], d2_send.at[2])
    sent(og.at[:, pl.ds(0, side), pl.ds(0, chunk // 2)], d2_send.at[3])
    sent(y_send.at[pl.ds(0, 3)], d3_send.at[0])
    out.wait()


def back(tp_size, cp_size, q, kv, w_o):
    rows, width = q.shape
    group = width // HEAD_DIM
    model_width = w_o.shape[1]
    side = 4
    cols = model_width // side
    chunk = rows // tp_size
    any_space = pl.BlockSpec(memory_space=pl.ANY)
    dma = pltpu.SemaphoreType.DMA
    bf16 = jnp.bfloat16
    flops = 4 * rows * width * (kv.shape[0] // 2) + 2 * rows * width * model_width
    return pl.pallas_call(
        functools.partial(back_kernel, tp_size, cp_size),
        out_shape=jax.ShapeDtypeStruct((chunk, model_width), bf16),
        in_specs=[any_space] * 3,
        out_specs=any_space,
        scratch_shapes=[
            pltpu.VMEM((rows, width), bf16),
            pltpu.VMEM(kv.shape, bf16),
            pltpu.VMEM((w_o.shape[0] * tp_size, cols), bf16),
            pltpu.VMEM((w_o.shape[0] // cp_size, model_width), bf16),
            pltpu.VMEM((side, tp_size, chunk, width), bf16),
            pltpu.VMEM((side, side, chunk, width), bf16),
            pltpu.VMEM((side, chunk, cols), bf16),
            pltpu.VMEM((chunk, model_width), bf16),
        ] + [pltpu.VMEM((group, SUB, 128), jnp.float32) for _ in range(3)] + [
            dma((3,)), dma((8,)), dma((8,)), dma((1,)), dma((side,)), dma((4,)), dma((side, 6)), dma((1,)), dma((1,)),
        ],
        compiler_params=pltpu.CompilerParams(collective_id=1, has_side_effects=True, vmem_limit_bytes=56 * 1024 * 1024),
        cost_estimate=pl.CostEstimate(flops=flops, bytes_accessed=kv.size * 2, transcendentals=flops // 512),
        name="back",
    )(q, kv, w_o)


def solution(mesh):
    cp_size = mesh.shape["cp"]
    tp_size = mesh.shape["tp"]
    row_spec = P(("dp", "cp", "tp"), None)

    def local_layer(x_loc, w_q, w_k, w_v, w_o):
        q_own, kv_all = front(tp_size, cp_size, x_loc, w_q, w_k, w_v)
        return back(tp_size, cp_size, q_own, kv_all, w_o)

    return jax.shard_map(local_layer, mesh=mesh, in_specs=(row_spec, P(None, "tp"), P(None, "tp"), P(None, "tp"), P("tp", None)), out_specs=row_spec, check_vma=False)
```

```python
import functools

import jax
import jax.numpy as jnp
from jax import lax
from jax.experimental import pallas as pl
from jax.experimental.pallas import tpu as pltpu
from jax.sharding import PartitionSpec as P

HEAD_DIM = 128
LOG2E = 1.4426950408889634
NT = (((1,), (1,)), ((), ()))
SUB = 512


MESH = pl.DeviceIdType.MESH
X_SUB = 2


def layer_kernel(tp_size, cp_size, x_hbm, wq_hbm, wk_hbm, wv_hbm, wo_hbm, y_hbm, xg, w_in, q_buf, kv, w_buf, wo_buf, og, o_buf, y_send, y_all, relay, acc_ref, m_ref, l_ref, load_sem, ring_send, ring_recv, kv_send, left_recv, right_recv, far_recv, pair_recv, w_send, w_recv, d1_send, d1_recv, d2_send, d2_recv, d3_send, d3_recv, relay_recv):
    tp = lax.axis_index("tp")
    cp = lax.axis_index("cp")
    side = 4
    zi, yi = tp // side, lax.rem(tp, side)
    chip, core = cp // 2, lax.rem(cp, 2)
    n_chip = cp_size // 2
    rows = x_hbm.shape[0]
    piece = q_buf.shape[0] // 2
    group = q_buf.shape[1] // HEAD_DIM
    chunk = SUB // side
    slab = wo_buf.shape[0]
    head_rows = slab * cp_size
    cols = w_buf.shape[1]
    coef = LOG2E * HEAD_DIM ** -0.5
    up = lax.rem(zi + 1, side)
    down = lax.rem(zi + side - 1, side)
    z_far = lax.rem(zi + 2, side)
    block = rows * tp_size
    part = rows // 4
    sub = part // X_SUB
    q_width = wq_hbm.shape[1]
    k_width = wk_hbm.shape[1]
    pos = (zi * side + lax.rem(yi + zi, side), yi * side + lax.rem(zi + yi, side))

    def member(cycle, k):
        k = lax.rem(k + 2 * tp_size, tp_size)
        major = k // side
        minor = lax.rem(k - major + side, side)
        return major * side + minor if cycle == 0 else minor * side + major

    streams = [(0, 1), (0, -1), (1, 1), (1, -1)]
    nxt = [member(c, pos[c] + d) for c, d in streams]
    right = lax.rem(chip + 1, n_chip) * 2 + core
    left = lax.rem(chip + n_chip - 1, n_chip) * 2 + core
    far = lax.rem(chip + 2, n_chip) * 2 + core
    pair = cp + 1 - 2 * core
    ahead = jnp.where(core == 0, right, left)
    behind = jnp.where(core == 0, left, right)

    w_q = pltpu.make_async_copy(wq_hbm, w_in.at[:, pl.ds(0, q_width)], load_sem.at[0])
    w_k = pltpu.make_async_copy(wk_hbm, w_in.at[:, pl.ds(q_width, k_width)], load_sem.at[1])
    w_v = pltpu.make_async_copy(wv_hbm, w_in.at[:, pl.ds(q_width + k_width, k_width)], load_sem.at[2])
    own = pltpu.make_async_copy(x_hbm, xg.at[pl.ds(pl.multiple_of(tp * rows, rows), rows)], load_sem.at[3])
    load_w = pltpu.make_async_copy(wo_hbm.at[pl.ds(pl.multiple_of(cp * slab, slab), slab)], wo_buf, load_sem.at[4])
    own.start()
    w_q.start()
    w_k.start()
    w_v.start()
    load_w.start()

    barrier = pltpu.get_barrier_semaphore()
    for k in range(1, tp_size):
        pl.semaphore_signal(barrier, inc=1, device_id={"tp": lax.rem(tp + k, tp_size)}, device_id_type=MESH)
    for peer in (left, right, pair):
        pl.semaphore_signal(barrier, inc=1, device_id={"cp": peer}, device_id_type=MESH)
    pl.semaphore_wait(barrier, tp_size + 2)
    own.wait()

    def source(s, t):
        c, d = streams[s]
        return member(c, pos[c] - d * t)

    def move(src, dst, send_sem, recv_sem, axis, peer):
        return pltpu.make_async_remote_copy(src_ref=src, dst_ref=dst, send_sem=send_sem, recv_sem=recv_sem, device_id={axis: peer}, device_id_type=MESH)

    def kv_rows(owner, s, t):
        return kv.at[pl.ds(pl.multiple_of(owner * block + source(s, t) * rows + s * part, part), part)]

    def got(ref, recv_sem):
        move(ref, ref, w_send.at[0], recv_sem, "cp", pair).wait_recv()

    def sent(ref, send_sem):
        move(ref, ref, send_sem, w_recv.at[0], "cp", pair).wait_send()

    kv_unit = kv.at[pl.ds(0, rows)]

    def kv_own(u):
        for s in range(4):
            at = kv_rows(cp, s, u)
            move(at, at, kv_send.at[0], left_recv.at[u], "cp", right).start()
            move(at, at, kv_send.at[1], right_recv.at[u], "cp", left).start()
            move(at, at, kv_send.at[2], pair_recv.at[0], "cp", pair).start()

    def kv_forward(u):
        got(kv_unit, left_recv.at[u])
        got(kv_unit, right_recv.at[u])
        for s in range(4):
            at = kv_rows(behind, s, u)
            move(at, at, kv_send.at[3], far_recv.at[u], "cp", ahead).start()
            at = kv_rows(left, s, u)
            move(at, at, kv_send.at[4], pair_recv.at[1], "cp", pair).start()
            at = kv_rows(right, s, u)
            move(at, at, kv_send.at[5], pair_recv.at[2], "cp", pair).start()

    def kv_far(u):
        got(kv_unit, far_recv.at[u])
        for s in range(4):
            at = kv_rows(far, s, u)
            move(at, at, kv_send.at[6], pair_recv.at[3], "cp", pair).start()

    def w_rows(owner, member):
        return w_buf.at[pl.ds(pl.multiple_of(owner * head_rows + member * slab, slab), slab)]

    def w_cols(quarter):
        return wo_buf.at[:, pl.ds(pl.multiple_of(quarter * cols, 128), cols)]

    own_w = pltpu.make_async_copy(w_cols(zi), w_rows(tp, cp), load_sem.at[5])

    def spread(k, _):
        peer = lax.rem(tp + k, tp_size)
        move(w_cols(peer // side), w_rows(tp, cp), w_send.at[0], w_recv.at[0], "tp", peer).start()
        return 0

    def step(t, _):
        @pl.when(t == tp_size - 1)
        def _():
            load_w.wait()
            own_w.start()
            lax.fori_loop(1, tp_size, spread, 0)

        for u in range(X_SUB):
            for s in range(4):
                at = xg.at[pl.ds(pl.multiple_of(source(s, t) * rows + s * part + u * sub, sub), sub)]

                @pl.when(t > 0)
                def _():
                    move(at, at, ring_send.at[s], ring_recv.at[s, t - 1, u], "tp", nxt[s]).wait_recv()

                @pl.when(t < tp_size - 1)
                def _():
                    move(at, at, ring_send.at[s], ring_recv.at[s, t, u], "tp", nxt[s]).start()

        @pl.when(t >= 1)
        def _():
            kv_own(t - 1)

        @pl.when(t >= 2)
        def _():
            kv_forward(t - 2)

        @pl.when(t >= 3)
        def _():
            kv_far(t - 3)

        @pl.when(t == 0)
        def _():
            w_q.wait()
            w_k.wait()
            w_v.wait()

        offs = [pl.multiple_of(source(s, t) * rows + s * part, part) for s in range(4)]
        lhs = jnp.concatenate([xg[pl.ds(o, part), :] for o in offs], axis=0)
        res = jnp.dot(lhs, w_in[...], preferred_element_type=jnp.float32).astype(jnp.bfloat16)
        for s in range(4):
            q_buf[pl.ds(offs[s], part), :] = res[s * part:(s + 1) * part, 0:q_width]
            kv[pl.ds(pl.multiple_of(cp * block + offs[s], part), part), :] = res[s * part:(s + 1) * part, q_width:]
        return 0

    lax.fori_loop(0, tp_size, step, 0)
    kv_own(tp_size - 1)
    kv_forward(tp_size - 2)
    kv_far(tp_size - 3)

    def w_share():
        own_w.wait()
        got(w_buf.at[pl.ds(0, (tp_size - 1) * slab)], w_recv.at[0])

        def one(s, _):
            ref = w_rows(s, cp)
            move(ref, ref, w_send.at[1], w_recv.at[1], "cp", right).start()
            move(ref, ref, w_send.at[2], w_recv.at[2], "cp", left).start()
            move(ref, ref, w_send.at[3], w_recv.at[4], "cp", pair).start()
            return 0

        lax.fori_loop(0, tp_size, one, 0)

    w_part = w_buf.at[pl.ds(0, tp_size * slab)]

    def w_pass():
        got(w_part, w_recv.at[1])
        got(w_part, w_recv.at[2])

        def one(s, _):
            ref = w_rows(s, behind)
            move(ref, ref, w_send.at[4], w_recv.at[3], "cp", ahead).start()
            ref = w_rows(s, left)
            move(ref, ref, w_send.at[5], w_recv.at[5], "cp", pair).start()
            ref = w_rows(s, right)
            move(ref, ref, w_send.at[6], w_recv.at[6], "cp", pair).start()
            return 0

        lax.fori_loop(0, tp_size, one, 0)

    def w_last():
        got(w_part, w_recv.at[3])

        def one(s, _):
            ref = w_rows(s, far)
            move(ref, ref, w_send.at[7], w_recv.at[7], "cp", pair).start()
            return 0

        lax.fori_loop(0, tp_size, one, 0)

    def lane_sum(p):
        total = p[:, 0:128]
        for c in range(1, p.shape[1] // 128):
            total = total + p[:, c * 128:(c + 1) * 128]
        return total

    def scores(i, g, base, width):
        qs = q_buf[pl.ds(pl.multiple_of(i * SUB, SUB), SUB), g * HEAD_DIM:(g + 1) * HEAD_DIM]
        ks = kv[pl.ds(pl.multiple_of(base, SUB), width), 0:HEAD_DIM]
        return lax.dot_general(qs, ks, NT, preferred_element_type=jnp.float32)

    def values(p, base, width):
        vs = kv[pl.ds(pl.multiple_of(base, SUB), width), HEAD_DIM:2 * HEAD_DIM]
        return jnp.dot(p.astype(jnp.bfloat16), vs, preferred_element_type=jnp.float32)

    def diag(i, s):
        width = (s + 1) * SUB
        base = cp * 2 * piece + (i // 2) * piece
        for g in range(group):
            sc = scores(i, g, base, width)
            row = lax.broadcasted_iota(jnp.int32, (SUB, width), 0) + s * SUB
            col = lax.broadcasted_iota(jnp.int32, (SUB, width), 1)
            sc = jnp.where(row >= col, sc, -jnp.inf)
            top = jnp.max(sc, axis=1, keepdims=True) * coef
            p = jnp.exp2(sc * coef - top)
            m_ref[g] = jnp.broadcast_to(top, (SUB, 128))
            l_ref[g] = lane_sum(p)
            acc_ref[g] = values(p, base, width)

    def d1(i, k):
        peer = lax.rem(yi + k, side)
        return move(o_buf.at[i, peer], og.at[i, tp], d1_send.at[0], d1_recv.at[i], "tp", zi * side + peer)

    def tile_part(i, z, half):
        return og.at[i, pl.ds(z * side, side), pl.ds(half * (chunk // 2), chunk // 2)]

    def d2(i, z, half, send, recv, peer):
        ref = tile_part(i, z, half)
        return move(ref, ref, d2_send.at[send], d2_recv.at[i, recv], "tp", peer * side + yi)

    def gather_start(i):
        got(og.at[i, pl.ds(0, side - 1)], d1_recv.at[i])
        d2(i, zi, 0, 0, 0, up).start()
        d2(i, zi, 1, 1, 2, down).start()
        d2(i, zi, 1, 0, 1, up).start()
        d2(i, zi, 0, 1, 3, down).start()

    def gather_pass(i):
        got(tile_part(i, down, 0), d2_recv.at[i, 0])
        d2(i, down, 0, 2, 4, up).start()
        got(tile_part(i, up, 1), d2_recv.at[i, 2])
        d2(i, up, 1, 3, 5, down).start()

    def gather_end(i):
        got(tile_part(i, down, 1), d2_recv.at[i, 1])
        got(tile_part(i, up, 0), d2_recv.at[i, 3])
        got(tile_part(i, z_far, 0), d2_recv.at[i, 4])
        got(tile_part(i, z_far, 1), d2_recv.at[i, 5])

    y_mine = y_all.at[:, pl.ds(pl.multiple_of(zi * cols, 128), cols)]

    def project(i):
        lhs = jnp.concatenate([og[i, s] for s in range(tp_size)], axis=1)
        y_send[i] = jnp.dot(lhs, w_buf[...], preferred_element_type=jnp.float32).astype(jnp.bfloat16)

    half = chunk // 2

    def y_part(h, z):
        return y_all.at[pl.ds(h * half, half), pl.ds(pl.multiple_of(z * cols, 128), cols)]

    def deliver(i):
        dist = lax.rem(i - zi + side, side)

        @pl.when(lax.rem(dist, 2) == 1)
        def _():
            move(y_send.at[i], y_mine, d3_send.at[0], d3_recv.at[0], "tp", i * side + yi).start()

        @pl.when(dist == 2)
        def _():
            move(y_send.at[i, pl.ds(0, half)], relay.at[0], d3_send.at[1], relay_recv.at[0], "tp", up * side + yi).start()
            move(y_send.at[i, pl.ds(half, half)], relay.at[1], d3_send.at[1], relay_recv.at[1], "tp", down * side + yi).start()

        @pl.when(dist == 0)
        def _():
            y_all[:, pl.ds(pl.multiple_of(zi * cols, 128), cols)] = y_send[i]

    def hand_on(i):
        dist = lax.rem(i - zi + side, side)

        @pl.when(dist == 1)
        def _():
            got(relay.at[0], relay_recv.at[0])
            move(relay.at[0], y_part(0, down), d3_send.at[2], d3_recv.at[1], "tp", up * side + yi).start()

        @pl.when(dist == 3)
        def _():
            got(relay.at[1], relay_recv.at[1])
            move(relay.at[1], y_part(1, up), d3_send.at[3], d3_recv.at[2], "tp", down * side + yi).start()

    def tile(i, _):
        is_low = i < 2
        count = jnp.where(is_low, cp, 2 * cp_size - 1 - cp)
        before = jnp.where(is_low, i * cp, 2 * cp + (i - 2) * (2 * cp_size - 1 - cp))

        @pl.when(lax.rem(i, 2) == 0)
        def _():
            diag(i, 0)

        @pl.when(lax.rem(i, 2) == 1)
        def _():
            diag(i, 1)

        @pl.when(i == 0)
        def _():
            kv_forward(tp_size - 1)
            kv_far(tp_size - 2)
            kv_far(tp_size - 1)
            for k in range(4):
                got(kv.at[pl.ds(0, block)], pair_recv.at[k])

        @pl.when(i == 2)
        def _():
            gather_start(0)
            gather_start(1)

        @pl.when(i == 3)
        def _():
            gather_start(2)

        def full(j, _):
            first = j < cp_size
            base = jnp.where(first, j * 2 * piece, (2 * cp_size - 1 - j) * 2 * piece + piece)
            turn = before + j
            pl.when(turn == 6)(w_share)
            pl.when(turn == 21)(w_pass)
            pl.when(turn == 28)(w_last)
            nxt = scores(i, 0, base, piece)
            for g in range(group):
                sc = nxt
                if g + 1 < group:
                    nxt = scores(i, g + 1, base, piece)
                m_old = m_ref[g]
                top = jnp.max(sc, axis=1, keepdims=True) * coef
                m_new = jnp.maximum(m_old, top)
                scale = jnp.exp2(m_old - m_new)
                p = jnp.exp2(sc * coef - m_new[:, 0:1])
                m_ref[g] = m_new
                l_ref[g] = l_ref[g] * scale + lane_sum(p)
                acc_ref[g] = acc_ref[g] * scale + values(p, base, piece)
            return 0

        early = jnp.minimum(count, 6)
        lax.fori_loop(0, early, full, 0)

        @pl.when(i == 2)
        def _():
            gather_pass(0)
            gather_pass(1)

        @pl.when(i == 3)
        def _():
            gather_pass(2)

        lax.fori_loop(early, count, full, 0)
        for g in range(group):
            total = jnp.sum(l_ref[g], axis=1, keepdims=True)
            out = (acc_ref[g] / total).astype(jnp.bfloat16)
            for k in range(side):
                o_buf[i, k, :, g * HEAD_DIM:(g + 1) * HEAD_DIM] = out[k * chunk:(k + 1) * chunk]
        og[i, tp] = o_buf[i, yi]
        for k in range(1, side):
            d1(i, k).start()
        return 0

    lax.fori_loop(0, side, tile, 0)

    gather_start(3)
    for k in range(4, 8):
        got(w_part, w_recv.at[k])
    for i in range(3):
        gather_end(i)
    lax.fori_loop(0, 3, lambda i, c: (project(i), c)[1], 0)
    gather_pass(3)
    for i in range(3):
        deliver(i)
    gather_end(3)
    project(3)
    deliver(3)
    for i in range(4):
        hand_on(i)
    got(y_all.at[:, pl.ds(0, 2 * cols)], d3_recv.at[0])
    got(relay.at[0], d3_recv.at[1])
    got(relay.at[1], d3_recv.at[2])
    out = pltpu.make_async_copy(y_all, y_hbm, load_sem.at[0])
    out.start()
    for s in range(4):
        sent(xg.at[pl.ds(0, (tp_size - 1) * part)], ring_send.at[s])
    for k in range(7):
        sent(kv.at[pl.ds(0, block)], kv_send.at[k])
    sent(w_buf.at[pl.ds(0, (tp_size - 1) * slab)], w_send.at[0])
    for k in range(1, 8):
        sent(w_part, w_send.at[k])
    sent(o_buf.at[:, pl.ds(0, side - 1)], d1_send.at[0])
    sent(og.at[:, pl.ds(0, side)], d2_send.at[0])
    sent(og.at[:, pl.ds(0, side)], d2_send.at[1])
    sent(og.at[:, pl.ds(0, side), pl.ds(0, chunk // 2)], d2_send.at[2])
    sent(og.at[:, pl.ds(0, side), pl.ds(0, chunk // 2)], d2_send.at[3])
    sent(y_send.at[pl.ds(0, 2)], d3_send.at[0])
    sent(y_send.at[0], d3_send.at[1])
    sent(relay.at[0], d3_send.at[2])
    sent(relay.at[1], d3_send.at[3])
    out.wait()


def layer(tp_size, cp_size, x_loc, w_q, w_k, w_v, w_o):
    rows, depth = x_loc.shape
    block = rows * tp_size
    q_width = w_q.shape[1]
    kv_width = w_k.shape[1] + w_v.shape[1]
    group = q_width // HEAD_DIM
    model_width = w_o.shape[1]
    side = 4
    cols = model_width // side
    any_space = pl.BlockSpec(memory_space=pl.ANY)
    dma = pltpu.SemaphoreType.DMA
    bf16 = jnp.bfloat16
    flops = 2 * block * depth * (2 * q_width + kv_width) + 2 * block * q_width * block * cp_size
    return pl.pallas_call(
        functools.partial(layer_kernel, tp_size, cp_size),
        out_shape=jax.ShapeDtypeStruct((rows, model_width), bf16),
        in_specs=[any_space] * 5,
        out_specs=any_space,
        scratch_shapes=[
            pltpu.VMEM((block, depth), bf16),
            pltpu.VMEM((depth, q_width + kv_width), bf16),
            pltpu.VMEM((block, q_width), bf16),
            pltpu.VMEM((block * cp_size, kv_width), bf16),
            pltpu.VMEM((w_o.shape[0] * tp_size, cols), bf16),
            pltpu.VMEM((w_o.shape[0] // cp_size, model_width), bf16),
            pltpu.VMEM((side, tp_size, rows, q_width), bf16),
            pltpu.VMEM((side, side, rows, q_width), bf16),
            pltpu.VMEM((side, rows, cols), bf16),
            pltpu.VMEM((rows, model_width), bf16),
            pltpu.VMEM((2, rows // 2, cols), bf16),
        ] + [pltpu.VMEM((group, SUB, 128), jnp.float32) for _ in range(3)] + [
            dma((6,)), dma((4,)), dma((4, tp_size - 1, X_SUB)), dma((7,)), dma((tp_size,)), dma((tp_size,)), dma((tp_size,)), dma((4,)),
            dma((8,)), dma((8,)), dma((1,)), dma((side,)), dma((4,)), dma((side, 6)), dma((4,)), dma((3,)), dma((2,)),
        ],
        compiler_params=pltpu.CompilerParams(collective_id=0, has_side_effects=True, vmem_limit_bytes=67043328),
        cost_estimate=pl.CostEstimate(flops=flops, bytes_accessed=block * depth * 2, transcendentals=0),
        name="layer",
    )(x_loc, w_q, w_k, w_v, w_o)


def solution(mesh):
    cp_size = mesh.shape["cp"]
    tp_size = mesh.shape["tp"]
    row_spec = P(("dp", "cp", "tp"), None)
    local_layer = functools.partial(layer, tp_size, cp_size)
    return jax.shard_map(local_layer, mesh=mesh, in_specs=(row_spec, P(None, "tp"), P(None, "tp"), P(None, "tp"), P("tp", None)), out_specs=row_spec, check_vma=False)
```

```python
import functools

import jax
import jax.numpy as jnp
from jax import lax
from jax.experimental import pallas as pl
from jax.experimental.pallas import tpu as pltpu
from jax.sharding import PartitionSpec as P

HEAD_DIM = 128
LOG2E = 1.4426950408889634
NT = (((1,), (1,)), ((), ()))
SUB = 512


MESH = pl.DeviceIdType.MESH
X_SUB = 2


def layer_kernel(tp_size, cp_size, x_hbm, wq_hbm, wk_hbm, wv_hbm, wo_hbm, y_hbm, xg, w_in, q_buf, kv, w_buf, wo_buf, og, o_buf, y_send, y_all, relay, acc_ref, m_ref, l_ref, x_ref, s_even, s_odd, load_sem, ring_send, ring_recv, kv_send, left_recv, right_recv, far_recv, pair_recv, w_send, w_recv, d1_send, d1_recv, d2_send, d2_recv, d3_send, d3_recv, relay_recv):
    tp = lax.axis_index("tp")
    cp = lax.axis_index("cp")
    side = 4
    zi, yi = tp // side, lax.rem(tp, side)
    chip, core = cp // 2, lax.rem(cp, 2)
    n_chip = cp_size // 2
    rows = x_hbm.shape[0]
    piece = q_buf.shape[0] // 2
    group = q_buf.shape[1] // HEAD_DIM
    chunk = SUB // side
    slab = wo_buf.shape[0]
    head_rows = slab * cp_size
    cols = w_buf.shape[1]
    coef = LOG2E * HEAD_DIM ** -0.5
    up = lax.rem(zi + 1, side)
    down = lax.rem(zi + side - 1, side)
    z_far = lax.rem(zi + 2, side)
    block = rows * tp_size
    part = rows // 4
    sub = part // X_SUB
    q_width = wq_hbm.shape[1]
    k_width = wk_hbm.shape[1]
    pos = (zi * side + lax.rem(yi + zi, side), yi * side + lax.rem(zi + yi, side))

    def member(cycle, k):
        k = lax.rem(k + 2 * tp_size, tp_size)
        major = k // side
        minor = lax.rem(k - major + side, side)
        return major * side + minor if cycle == 0 else minor * side + major

    streams = [(0, 1), (0, -1), (1, 1), (1, -1)]
    nxt = [member(c, pos[c] + d) for c, d in streams]
    right = lax.rem(chip + 1, n_chip) * 2 + core
    left = lax.rem(chip + n_chip - 1, n_chip) * 2 + core
    far = lax.rem(chip + 2, n_chip) * 2 + core
    pair = cp + 1 - 2 * core
    ahead = jnp.where(core == 0, right, left)
    behind = jnp.where(core == 0, left, right)

    w_q = pltpu.make_async_copy(wq_hbm, w_in.at[:, pl.ds(0, q_width)], load_sem.at[0])
    w_k = pltpu.make_async_copy(wk_hbm, w_in.at[:, pl.ds(q_width, k_width)], load_sem.at[1])
    w_v = pltpu.make_async_copy(wv_hbm, w_in.at[:, pl.ds(q_width + k_width, k_width)], load_sem.at[2])
    own = pltpu.make_async_copy(x_hbm, xg.at[pl.ds(pl.multiple_of(tp * rows, rows), rows)], load_sem.at[3])
    load_w = pltpu.make_async_copy(wo_hbm.at[pl.ds(pl.multiple_of(cp * slab, slab), slab)], wo_buf, load_sem.at[4])
    own.start()
    w_q.start()
    w_k.start()
    w_v.start()
    load_w.start()

    barrier = pltpu.get_barrier_semaphore()
    for k in range(1, tp_size):
        pl.semaphore_signal(barrier, inc=1, device_id={"tp": lax.rem(tp + k, tp_size)}, device_id_type=MESH)
    for peer in (left, right, pair):
        pl.semaphore_signal(barrier, inc=1, device_id={"cp": peer}, device_id_type=MESH)
    pl.semaphore_wait(barrier, tp_size + 2)
    own.wait()

    def source(s, t):
        c, d = streams[s]
        return member(c, pos[c] - d * t)

    def move(src, dst, send_sem, recv_sem, axis, peer):
        return pltpu.make_async_remote_copy(src_ref=src, dst_ref=dst, send_sem=send_sem, recv_sem=recv_sem, device_id={axis: peer}, device_id_type=MESH)

    def kv_rows(owner, s, t):
        return kv.at[pl.ds(pl.multiple_of(owner * block + source(s, t) * rows + s * part, part), part)]

    def got(ref, recv_sem):
        move(ref, ref, w_send.at[0], recv_sem, "cp", pair).wait_recv()

    def sent(ref, send_sem):
        move(ref, ref, send_sem, w_recv.at[0], "cp", pair).wait_send()

    kv_unit = kv.at[pl.ds(0, rows)]

    def kv_own(u):
        for s in range(4):
            at = kv_rows(cp, s, u)
            move(at, at, kv_send.at[0], left_recv.at[u], "cp", right).start()
            move(at, at, kv_send.at[1], right_recv.at[u], "cp", left).start()
            move(at, at, kv_send.at[2], pair_recv.at[0], "cp", pair).start()

    def kv_forward(u):
        got(kv_unit, left_recv.at[u])
        got(kv_unit, right_recv.at[u])
        for s in range(4):
            at = kv_rows(behind, s, u)
            move(at, at, kv_send.at[3], far_recv.at[u], "cp", ahead).start()
            at = kv_rows(left, s, u)
            move(at, at, kv_send.at[4], pair_recv.at[1], "cp", pair).start()
            at = kv_rows(right, s, u)
            move(at, at, kv_send.at[5], pair_recv.at[2], "cp", pair).start()

    def kv_far(u):
        got(kv_unit, far_recv.at[u])
        for s in range(4):
            at = kv_rows(far, s, u)
            move(at, at, kv_send.at[6], pair_recv.at[3], "cp", pair).start()

    def w_rows(owner, member):
        return w_buf.at[pl.ds(pl.multiple_of(owner * head_rows + member * slab, slab), slab)]

    def w_cols(quarter):
        return wo_buf.at[:, pl.ds(pl.multiple_of(quarter * cols, 128), cols)]

    own_w = pltpu.make_async_copy(w_cols(zi), w_rows(tp, cp), load_sem.at[5])

    n_group = 4
    per_group = tp_size // n_group

    def w_fetch():
        for k in range(1, tp_size):
            peer = lax.rem(tp + k, tp_size)
            move(w_cols(peer // side), w_rows(tp, cp), w_send.at[0], w_recv.at[k // per_group], "tp", peer).start()

    def w_sources(grp):
        return [lax.rem(tp - k + tp_size, tp_size) for k in range(grp * per_group, (grp + 1) * per_group)]

    w_group = w_buf.at[pl.ds(0, per_group * slab)]

    def step(t, _):
        @pl.when(t == tp_size - 1)
        def _():
            load_w.wait()
            own_w.start()
            w_fetch()

        for u in range(X_SUB):
            for s in range(4):
                at = xg.at[pl.ds(pl.multiple_of(source(s, t) * rows + s * part + u * sub, sub), sub)]

                @pl.when(t > 0)
                def _():
                    move(at, at, ring_send.at[s], ring_recv.at[s, t - 1, u], "tp", nxt[s]).wait_recv()

                @pl.when(t < tp_size - 1)
                def _():
                    move(at, at, ring_send.at[s], ring_recv.at[s, t, u], "tp", nxt[s]).start()

        @pl.when(t >= 1)
        def _():
            kv_own(t - 1)

        @pl.when(t >= 2)
        def _():
            kv_forward(t - 2)

        @pl.when(t >= 3)
        def _():
            kv_far(t - 3)

        @pl.when(t == 0)
        def _():
            w_q.wait()
            w_k.wait()
            w_v.wait()

        offs = [pl.multiple_of(source(s, t) * rows + s * part, part) for s in range(4)]
        lhs = jnp.concatenate([xg[pl.ds(o, part), :] for o in offs], axis=0)
        res = jnp.dot(lhs, w_in[...], preferred_element_type=jnp.float32).astype(jnp.bfloat16)
        for s in range(4):
            q_buf[pl.ds(offs[s], part), :] = res[s * part:(s + 1) * part, 0:q_width]
            kv[pl.ds(pl.multiple_of(cp * block + offs[s], part), part), :] = res[s * part:(s + 1) * part, q_width:]
        return 0

    lax.fori_loop(0, tp_size, step, 0)
    kv_own(tp_size - 1)
    kv_forward(tp_size - 2)
    kv_far(tp_size - 3)

    def w_share(grp):
        if grp == 0:
            own_w.wait()
            got(w_buf.at[pl.ds(0, (per_group - 1) * slab)], w_recv.at[0])
        else:
            got(w_group, w_recv.at[grp])
        for o in w_sources(grp):
            ref = w_rows(o, cp)
            move(ref, ref, w_send.at[1], w_recv.at[4 + grp], "cp", right).start()
            move(ref, ref, w_send.at[2], w_recv.at[8 + grp], "cp", left).start()
            move(ref, ref, w_send.at[3], w_recv.at[16], "cp", pair).start()

    def w_pass(grp):
        got(w_group, w_recv.at[4 + grp])
        got(w_group, w_recv.at[8 + grp])
        for o in w_sources(grp):
            ref = w_rows(o, behind)
            move(ref, ref, w_send.at[4], w_recv.at[12 + grp], "cp", ahead).start()
            ref = w_rows(o, left)
            move(ref, ref, w_send.at[5], w_recv.at[17], "cp", pair).start()
            ref = w_rows(o, right)
            move(ref, ref, w_send.at[6], w_recv.at[18], "cp", pair).start()

    def w_last(grp):
        got(w_group, w_recv.at[12 + grp])
        for o in w_sources(grp):
            ref = w_rows(o, far)
            move(ref, ref, w_send.at[7], w_recv.at[19], "cp", pair).start()

    w_part = w_buf.at[pl.ds(0, tp_size * slab)]

    def fold(x, op):
        total = x[0:8]
        for c in range(1, x.shape[0] // 8):
            total = op(total, x[c * 8:(c + 1) * 8])
        return total

    def scores(i, g, base, width):
        qs = q_buf[pl.ds(pl.multiple_of(i * SUB, SUB), SUB), g * HEAD_DIM:(g + 1) * HEAD_DIM]
        ks = kv[pl.ds(pl.multiple_of(base, SUB), width), 0:HEAD_DIM]
        return lax.dot_general(ks, qs, NT, preferred_element_type=jnp.float32)

    def values(p, base, width):
        vs = kv[pl.ds(pl.multiple_of(base, SUB), width), HEAD_DIM:2 * HEAD_DIM]
        return jnp.dot(vs.T, p, preferred_element_type=jnp.float32)

    def diag(i, s):
        width = (s + 1) * SUB
        base = cp * 2 * piece + (i // 2) * piece
        for g in range(group):
            sc = scores(i, g, base, width)
            key = lax.broadcasted_iota(jnp.int32, (width, SUB), 0)
            query = lax.broadcasted_iota(jnp.int32, (width, SUB), 1) + s * SUB
            sc = jnp.where(query >= key, sc, -jnp.inf)
            top = jnp.max(sc, axis=0, keepdims=True) * coef
            p = jnp.exp2(sc * coef - top)
            m_ref[g, 0:1, :] = top
            l_ref[g] = fold(p, jnp.add)
            acc_ref[g] = values(p.astype(jnp.bfloat16), base, width)

    def d1(i, k):
        peer = lax.rem(yi + k, side)
        return move(o_buf.at[i, peer], og.at[i, tp], d1_send.at[0], d1_recv.at[i], "tp", zi * side + peer)

    def tile_part(i, z, half):
        return og.at[i, pl.ds(z * side, side), pl.ds(half * (chunk // 2), chunk // 2)]

    def d2(i, z, half, send, recv, peer):
        ref = tile_part(i, z, half)
        return move(ref, ref, d2_send.at[send], d2_recv.at[i, recv], "tp", peer * side + yi)

    def gather_start(i):
        got(og.at[i, pl.ds(0, side - 1)], d1_recv.at[i])
        d2(i, zi, 0, 0, 0, up).start()
        d2(i, zi, 1, 1, 2, down).start()
        d2(i, zi, 1, 0, 1, up).start()
        d2(i, zi, 0, 1, 3, down).start()

    def gather_pass(i):
        got(tile_part(i, down, 0), d2_recv.at[i, 0])
        d2(i, down, 0, 2, 4, up).start()
        got(tile_part(i, up, 1), d2_recv.at[i, 2])
        d2(i, up, 1, 3, 5, down).start()

    def gather_end(i):
        got(tile_part(i, down, 1), d2_recv.at[i, 1])
        got(tile_part(i, up, 0), d2_recv.at[i, 3])
        got(tile_part(i, z_far, 0), d2_recv.at[i, 4])
        got(tile_part(i, z_far, 1), d2_recv.at[i, 5])

    y_mine = y_all.at[:, pl.ds(pl.multiple_of(zi * cols, 128), cols)]

    def project(i):
        lhs = jnp.concatenate([og[i, s] for s in range(tp_size)], axis=1)
        y_send[i] = jnp.dot(lhs, w_buf[...], preferred_element_type=jnp.float32).astype(jnp.bfloat16)

    half = chunk // 2

    def y_part(h, z):
        return y_all.at[pl.ds(h * half, half), pl.ds(pl.multiple_of(z * cols, 128), cols)]

    def deliver(i):
        dist = lax.rem(i - zi + side, side)

        @pl.when(lax.rem(dist, 2) == 1)
        def _():
            move(y_send.at[i], y_mine, d3_send.at[0], d3_recv.at[0], "tp", i * side + yi).start()

        @pl.when(dist == 2)
        def _():
            move(y_send.at[i, pl.ds(0, half)], relay.at[0], d3_send.at[1], relay_recv.at[0], "tp", up * side + yi).start()
            move(y_send.at[i, pl.ds(half, half)], relay.at[1], d3_send.at[1], relay_recv.at[1], "tp", down * side + yi).start()

        @pl.when(dist == 0)
        def _():
            y_all[:, pl.ds(pl.multiple_of(zi * cols, 128), cols)] = y_send[i]

    def hand_on(i):
        dist = lax.rem(i - zi + side, side)

        @pl.when(dist == 1)
        def _():
            got(relay.at[0], relay_recv.at[0])
            move(relay.at[0], y_part(0, down), d3_send.at[2], d3_recv.at[1], "tp", up * side + yi).start()

        @pl.when(dist == 3)
        def _():
            got(relay.at[1], relay_recv.at[1])
            move(relay.at[1], y_part(1, up), d3_send.at[3], d3_recv.at[2], "tp", down * side + yi).start()

    def tile(i, _):
        is_low = i < 2
        count = jnp.where(is_low, cp, 2 * cp_size - 1 - cp)
        before = jnp.where(is_low, i * cp, 2 * cp + (i - 2) * (2 * cp_size - 1 - cp))

        @pl.when(lax.rem(i, 2) == 0)
        def _():
            diag(i, 0)

        @pl.when(lax.rem(i, 2) == 1)
        def _():
            diag(i, 1)

        @pl.when(i == 0)
        def _():
            kv_forward(tp_size - 1)
            kv_far(tp_size - 2)
            kv_far(tp_size - 1)
            for k in range(4):
                got(kv.at[pl.ds(0, block)], pair_recv.at[k])

        def piece_base(j):
            return jnp.where(j < cp_size, j * 2 * piece, (2 * cp_size - 1 - j) * 2 * piece + piece)

        def look(g, base):
            ahead_sc = scores(i, g, base, piece)
            s_ref[g][...] = ahead_sc
            return ahead_sc

        def full(j, _):
            base = piece_base(j)
            later = piece_base(jnp.minimum(j + 1, count - 1))
            turn = before + j
            for grp, at in enumerate((0, 1, 3, 7)):
                pl.when(turn == at)(functools.partial(w_share, grp))
            for grp, at in enumerate((9, 14, 19, 24)):
                pl.when(turn == at)(functools.partial(w_pass, grp))
            for grp, at in enumerate((27, 29)):
                pl.when(turn == at)(functools.partial(w_last, grp))

            @pl.when(turn == low_turn)
            def _():
                gather_start(0)
                gather_start(1)

            @pl.when(turn == low_turn + 9)
            def _():
                gather_pass(0)
                gather_pass(1)

            @pl.when(turn == cp + 2 * cp_size + 2)
            def _():
                gather_start(2)

            @pl.when(turn == cp + 2 * cp_size + 6)
            def _():
                gather_pass(2)

            for g in range(group):
                top = jnp.max(x_ref[g], axis=0, keepdims=True) * coef
                m_old = m_ref[g, 0:1, :]
                m_new = jnp.maximum(m_old, top)
                scale = jnp.exp2(m_old - m_new)
                m_ref[g, 0:1, :] = m_new
                total = l_ref[g] * scale
                nxt = look((g + 1) % group, base if g + 1 < group else later)
                p = jnp.exp2(s_ref[g][...] * coef - m_new)
                total = total + fold(p, jnp.add)
                p = p.astype(jnp.bfloat16)
                peak = fold(nxt, jnp.maximum)
                acc_ref[g] = acc_ref[g] * scale + values(p, base, piece)
                l_ref[g] = total
                x_ref[(g + 1) % group] = peak
            return 0

        @pl.when(count > 0)
        def _():
            x_ref[0] = fold(look(0, piece_base(0)), jnp.maximum)

        lax.fori_loop(0, count, full, 0)
        for g in range(group):
            total = jnp.sum(l_ref[g], axis=0, keepdims=True)
            out = (acc_ref[g] / total).T.astype(jnp.bfloat16)
            for k in range(side):
                o_buf[i, k, :, g * HEAD_DIM:(g + 1) * HEAD_DIM] = out[k * chunk:(k + 1) * chunk]
        og[i, tp] = o_buf[i, yi]
        for k in range(1, side):
            d1(i, k).start()
        return 0

    low_turn = jnp.maximum(2 * cp + 2, 12)
    s_ref = (s_even, s_odd)
    lax.fori_loop(0, side, tile, 0)

    gather_start(3)
    w_last(2)
    w_last(3)
    for k in range(16, 20):
        got(w_part, w_recv.at[k])
    for i in range(3):
        gather_end(i)
    project(0)
    gather_pass(3)
    lax.fori_loop(1, 3, lambda i, c: (project(i), c)[1], 0)
    for i in range(3):
        deliver(i)
    gather_end(3)
    project(3)
    deliver(3)
    for i in range(4):
        hand_on(i)
    got(y_all.at[:, pl.ds(0, 2 * cols)], d3_recv.at[0])
    got(relay.at[0], d3_recv.at[1])
    got(relay.at[1], d3_recv.at[2])
    out = pltpu.make_async_copy(y_all, y_hbm, load_sem.at[0])
    out.start()
    for s in range(4):
        sent(xg.at[pl.ds(0, (tp_size - 1) * part)], ring_send.at[s])
    for k in range(7):
        sent(kv.at[pl.ds(0, block)], kv_send.at[k])
    sent(w_buf.at[pl.ds(0, (tp_size - 1) * slab)], w_send.at[0])
    for k in range(1, 8):
        sent(w_part, w_send.at[k])
    sent(o_buf.at[:, pl.ds(0, side - 1)], d1_send.at[0])
    sent(og.at[:, pl.ds(0, side)], d2_send.at[0])
    sent(og.at[:, pl.ds(0, side)], d2_send.at[1])
    sent(og.at[:, pl.ds(0, side), pl.ds(0, chunk // 2)], d2_send.at[2])
    sent(og.at[:, pl.ds(0, side), pl.ds(0, chunk // 2)], d2_send.at[3])
    sent(y_send.at[pl.ds(0, 2)], d3_send.at[0])
    sent(y_send.at[0], d3_send.at[1])
    sent(relay.at[0], d3_send.at[2])
    sent(relay.at[1], d3_send.at[3])
    out.wait()


def layer(tp_size, cp_size, x_loc, w_q, w_k, w_v, w_o):
    rows, depth = x_loc.shape
    block = rows * tp_size
    q_width = w_q.shape[1]
    kv_width = w_k.shape[1] + w_v.shape[1]
    group = q_width // HEAD_DIM
    model_width = w_o.shape[1]
    side = 4
    cols = model_width // side
    any_space = pl.BlockSpec(memory_space=pl.ANY)
    dma = pltpu.SemaphoreType.DMA
    bf16 = jnp.bfloat16
    flops = 2 * block * depth * (2 * q_width + kv_width) + 2 * block * q_width * block * cp_size
    return pl.pallas_call(
        functools.partial(layer_kernel, tp_size, cp_size),
        out_shape=jax.ShapeDtypeStruct((rows, model_width), bf16),
        in_specs=[any_space] * 5,
        out_specs=any_space,
        scratch_shapes=[
            pltpu.VMEM((block, depth), bf16),
            pltpu.VMEM((depth, q_width + kv_width), bf16),
            pltpu.VMEM((block, q_width), bf16),
            pltpu.VMEM((block * cp_size, kv_width), bf16),
            pltpu.VMEM((w_o.shape[0] * tp_size, cols), bf16),
            pltpu.VMEM((w_o.shape[0] // cp_size, model_width), bf16),
            pltpu.VMEM((side, tp_size, rows, q_width), bf16),
            pltpu.VMEM((side, side, rows, q_width), bf16),
            pltpu.VMEM((side, rows, cols), bf16),
            pltpu.VMEM((rows, model_width), bf16),
            pltpu.VMEM((2, rows // 2, cols), bf16),
        ] + [pltpu.VMEM((group, HEAD_DIM, SUB), jnp.float32)] + [pltpu.VMEM((group, 8, SUB), jnp.float32) for _ in range(3)] + [pltpu.VMEM((block // 2, SUB), jnp.float32) for _ in range(2)] + [
            dma((6,)), dma((4,)), dma((4, tp_size - 1, X_SUB)), dma((7,)), dma((tp_size,)), dma((tp_size,)), dma((tp_size,)), dma((4,)),
            dma((8,)), dma((20,)), dma((1,)), dma((side,)), dma((4,)), dma((side, 6)), dma((4,)), dma((3,)), dma((2,)),
        ],
        compiler_params=pltpu.CompilerParams(collective_id=0, has_side_effects=True, vmem_limit_bytes=67043328),
        cost_estimate=pl.CostEstimate(flops=flops, bytes_accessed=block * depth * 2, transcendentals=0),
        name="layer",
    )(x_loc, w_q, w_k, w_v, w_o)


def solution(mesh):
    cp_size = mesh.shape["cp"]
    tp_size = mesh.shape["tp"]
    row_spec = P(("dp", "cp", "tp"), None)
    local_layer = functools.partial(layer, tp_size, cp_size)
    return jax.shard_map(local_layer, mesh=mesh, in_specs=(row_spec, P(None, "tp"), P(None, "tp"), P(None, "tp"), P("tp", None)), out_specs=row_spec, check_vma=False)
```

```python
import functools

import jax
import jax.numpy as jnp
from jax import lax
from jax.experimental import pallas as pl
from jax.experimental.pallas import tpu as pltpu
from jax.sharding import PartitionSpec as P

HEAD_DIM = 128
LOG2E = 1.4426950408889634
NT = (((1,), (1,)), ((), ()))
SUB = 512


MESH = pl.DeviceIdType.MESH
X_SUB = 2


def layer_kernel(tp_size, cp_size, x_hbm, wq_hbm, wk_hbm, wv_hbm, wo_hbm, y_hbm, xg, w_in, q_buf, kv, w_buf, wo_buf, og, o_buf, y_send, y_all, relay, acc_ref, m_ref, l_ref, x_ref, s_even, s_odd, load_sem, ring_send, ring_recv, kv_send, left_recv, right_recv, far_recv, pair_recv, w_send, w_recv, d1_send, d1_recv, d2_send, d2_recv, d3_send, d3_recv, relay_recv):
    tp = lax.axis_index("tp")
    cp = lax.axis_index("cp")
    side = 4
    zi, yi = tp // side, lax.rem(tp, side)
    chip, core = cp // 2, lax.rem(cp, 2)
    n_chip = cp_size // 2
    rows = x_hbm.shape[0]
    piece = q_buf.shape[0] // 2
    group = q_buf.shape[1] // HEAD_DIM
    chunk = SUB // side
    slab = wo_buf.shape[0]
    head_rows = slab * cp_size
    cols = w_buf.shape[1]
    coef = LOG2E * HEAD_DIM ** -0.5
    up = lax.rem(zi + 1, side)
    down = lax.rem(zi + side - 1, side)
    z_far = lax.rem(zi + 2, side)
    block = rows * tp_size
    part = rows // 4
    sub = part // X_SUB
    q_width = wq_hbm.shape[1]
    k_width = wk_hbm.shape[1]
    pos = (zi * side + lax.rem(yi + zi, side), yi * side + lax.rem(zi + yi, side))

    def member(cycle, k):
        k = lax.rem(k + 2 * tp_size, tp_size)
        major = k // side
        minor = lax.rem(k - major + side, side)
        return major * side + minor if cycle == 0 else minor * side + major

    streams = [(0, 1), (0, -1), (1, 1), (1, -1)]
    nxt = [member(c, pos[c] + d) for c, d in streams]
    right = lax.rem(chip + 1, n_chip) * 2 + core
    left = lax.rem(chip + n_chip - 1, n_chip) * 2 + core
    far = lax.rem(chip + 2, n_chip) * 2 + core
    pair = cp + 1 - 2 * core
    ahead = jnp.where(core == 0, right, left)
    behind = jnp.where(core == 0, left, right)

    w_q = pltpu.make_async_copy(wq_hbm, w_in.at[:, pl.ds(0, q_width)], load_sem.at[0])
    w_k = pltpu.make_async_copy(wk_hbm, w_in.at[:, pl.ds(q_width, k_width)], load_sem.at[1])
    w_v = pltpu.make_async_copy(wv_hbm, w_in.at[:, pl.ds(q_width + k_width, k_width)], load_sem.at[2])
    own = pltpu.make_async_copy(x_hbm, xg.at[pl.ds(pl.multiple_of(tp * rows, rows), rows)], load_sem.at[3])
    load_w = pltpu.make_async_copy(wo_hbm.at[pl.ds(pl.multiple_of(cp * slab, slab), slab)], wo_buf, load_sem.at[4])
    own.start()
    w_q.start()
    w_k.start()
    w_v.start()
    load_w.start()

    barrier = pltpu.get_barrier_semaphore()
    for k in range(1, tp_size):
        pl.semaphore_signal(barrier, inc=1, device_id={"tp": lax.rem(tp + k, tp_size)}, device_id_type=MESH)
    for peer in (left, right, pair):
        pl.semaphore_signal(barrier, inc=1, device_id={"cp": peer}, device_id_type=MESH)
    pl.semaphore_wait(barrier, tp_size + 2)
    own.wait()

    def source(s, t):
        c, d = streams[s]
        return member(c, pos[c] - d * t)

    def move(src, dst, send_sem, recv_sem, axis, peer):
        return pltpu.make_async_remote_copy(src_ref=src, dst_ref=dst, send_sem=send_sem, recv_sem=recv_sem, device_id={axis: peer}, device_id_type=MESH)

    def kv_rows(owner, s, t):
        return kv.at[pl.ds(pl.multiple_of(owner * block + source(s, t) * rows + s * part, part), part)]

    def got(ref, recv_sem):
        move(ref, ref, w_send.at[0], recv_sem, "cp", pair).wait_recv()

    def sent(ref, send_sem):
        move(ref, ref, send_sem, w_recv.at[0], "cp", pair).wait_send()

    kv_unit = kv.at[pl.ds(0, rows)]

    def kv_own(u):
        for s in range(4):
            at = kv_rows(cp, s, u)
            move(at, at, kv_send.at[0], left_recv.at[u], "cp", right).start()
            move(at, at, kv_send.at[1], right_recv.at[u], "cp", left).start()
            move(at, at, kv_send.at[2], pair_recv.at[0], "cp", pair).start()

    def kv_forward(u):
        got(kv_unit, left_recv.at[u])
        got(kv_unit, right_recv.at[u])
        for s in range(4):
            at = kv_rows(behind, s, u)
            move(at, at, kv_send.at[3], far_recv.at[u], "cp", ahead).start()
            at = kv_rows(left, s, u)
            move(at, at, kv_send.at[4], pair_recv.at[1], "cp", pair).start()
            at = kv_rows(right, s, u)
            move(at, at, kv_send.at[5], pair_recv.at[2], "cp", pair).start()

    def kv_far(u):
        got(kv_unit, far_recv.at[u])
        for s in range(4):
            at = kv_rows(far, s, u)
            move(at, at, kv_send.at[6], pair_recv.at[3], "cp", pair).start()

    def w_rows(owner, member):
        return w_buf.at[pl.ds(pl.multiple_of(owner * head_rows + member * slab, slab), slab)]

    def w_cols(quarter):
        return wo_buf.at[:, pl.ds(pl.multiple_of(quarter * cols, 128), cols)]

    own_w = pltpu.make_async_copy(w_cols(zi), w_rows(tp, cp), load_sem.at[5])

    n_group = 4
    per_group = tp_size // n_group

    def w_fetch():
        for k in range(1, tp_size):
            peer = lax.rem(tp + k, tp_size)
            move(w_cols(peer // side), w_rows(tp, cp), w_send.at[0], w_recv.at[k // per_group], "tp", peer).start()

    def w_sources(grp):
        return [lax.rem(tp - k + tp_size, tp_size) for k in range(grp * per_group, (grp + 1) * per_group)]

    w_group = w_buf.at[pl.ds(0, per_group * slab)]

    def step(t, _):
        @pl.when(t == tp_size - 1)
        def _():
            load_w.wait()
            own_w.start()
            w_fetch()

        for u in range(X_SUB):
            for s in range(4):
                at = xg.at[pl.ds(pl.multiple_of(source(s, t) * rows + s * part + u * sub, sub), sub)]

                @pl.when(t > 0)
                def _():
                    move(at, at, ring_send.at[s], ring_recv.at[s, t - 1, u], "tp", nxt[s]).wait_recv()

                @pl.when(t < tp_size - 1)
                def _():
                    move(at, at, ring_send.at[s], ring_recv.at[s, t, u], "tp", nxt[s]).start()

        @pl.when(t >= 1)
        def _():
            kv_own(t - 1)

        @pl.when(t >= 2)
        def _():
            kv_forward(t - 2)

        @pl.when(t >= 3)
        def _():
            kv_far(t - 3)

        @pl.when(t == 0)
        def _():
            w_q.wait()
            w_k.wait()
            w_v.wait()

        offs = [pl.multiple_of(source(s, t) * rows + s * part, part) for s in range(4)]
        lhs = jnp.concatenate([xg[pl.ds(o, part), :] for o in offs], axis=0)
        res = jnp.dot(lhs, w_in[...], preferred_element_type=jnp.float32).astype(jnp.bfloat16)
        for s in range(4):
            q_buf[pl.ds(offs[s], part), :] = res[s * part:(s + 1) * part, 0:q_width]
            kv[pl.ds(pl.multiple_of(cp * block + offs[s], part), part), :] = res[s * part:(s + 1) * part, q_width:]
        return 0

    lax.fori_loop(0, tp_size, step, 0)
    kv_own(tp_size - 1)
    kv_forward(tp_size - 2)
    kv_far(tp_size - 3)

    def w_share(grp):
        if grp == 0:
            own_w.wait()
            got(w_buf.at[pl.ds(0, (per_group - 1) * slab)], w_recv.at[0])
        else:
            got(w_group, w_recv.at[grp])
        for o in w_sources(grp):
            ref = w_rows(o, cp)
            move(ref, ref, w_send.at[1], w_recv.at[4 + grp], "cp", right).start()
            move(ref, ref, w_send.at[2], w_recv.at[8 + grp], "cp", left).start()
            move(ref, ref, w_send.at[3], w_recv.at[16], "cp", pair).start()

    def w_pass(grp):
        got(w_group, w_recv.at[4 + grp])
        got(w_group, w_recv.at[8 + grp])
        for o in w_sources(grp):
            ref = w_rows(o, behind)
            move(ref, ref, w_send.at[4], w_recv.at[12 + grp], "cp", ahead).start()
            ref = w_rows(o, left)
            move(ref, ref, w_send.at[5], w_recv.at[17], "cp", pair).start()
            ref = w_rows(o, right)
            move(ref, ref, w_send.at[6], w_recv.at[18], "cp", pair).start()

    def w_last(grp):
        got(w_group, w_recv.at[12 + grp])
        for o in w_sources(grp):
            ref = w_rows(o, far)
            move(ref, ref, w_send.at[7], w_recv.at[19], "cp", pair).start()

    w_part = w_buf.at[pl.ds(0, tp_size * slab)]

    def fold(x, op):
        total = x[0:8]
        for c in range(1, x.shape[0] // 8):
            total = op(total, x[c * 8:(c + 1) * 8])
        return total

    def scores(i, g, base, width):
        qs = q_buf[pl.ds(pl.multiple_of(i * SUB, SUB), SUB), g * HEAD_DIM:(g + 1) * HEAD_DIM]
        ks = kv[pl.ds(pl.multiple_of(base, SUB), width), 0:HEAD_DIM]
        return lax.dot_general(ks, qs, NT, preferred_element_type=jnp.float32)

    def values(p, base, width):
        vs = kv[pl.ds(pl.multiple_of(base, SUB), width), HEAD_DIM:2 * HEAD_DIM]
        return jnp.dot(vs.T, p, preferred_element_type=jnp.float32)

    def diag(i, s):
        width = (s + 1) * SUB
        base = cp * 2 * piece + (i // 2) * piece
        for g in range(group):
            sc = scores(i, g, base, width)
            key = lax.broadcasted_iota(jnp.int32, (width, SUB), 0)
            query = lax.broadcasted_iota(jnp.int32, (width, SUB), 1) + s * SUB
            sc = jnp.where(query >= key, sc, -jnp.inf)
            top = jnp.max(sc, axis=0, keepdims=True) * coef
            p = jnp.exp2(sc * coef - top)
            m_ref[g, 0:1, :] = top
            l_ref[g] = fold(p, jnp.add)
            acc_ref[g] = values(p.astype(jnp.bfloat16), base, width)

    def d1(i, k):
        peer = lax.rem(yi + k, side)
        return move(o_buf.at[i, peer], og.at[i, tp], d1_send.at[0], d1_recv.at[i], "tp", zi * side + peer)

    def tile_part(i, z, half):
        return og.at[i, pl.ds(z * side, side), pl.ds(half * (chunk // 2), chunk // 2)]

    def d2(i, z, half, send, recv, peer):
        ref = tile_part(i, z, half)
        return move(ref, ref, d2_send.at[send], d2_recv.at[i, recv], "tp", peer * side + yi)

    def gather_start(i):
        got(og.at[i, pl.ds(0, side - 1)], d1_recv.at[i])
        d2(i, zi, 0, 0, 0, up).start()
        d2(i, zi, 1, 1, 2, down).start()
        d2(i, zi, 1, 0, 1, up).start()
        d2(i, zi, 0, 1, 3, down).start()

    def gather_pass(i):
        got(tile_part(i, down, 0), d2_recv.at[i, 0])
        d2(i, down, 0, 2, 4, up).start()
        got(tile_part(i, up, 1), d2_recv.at[i, 2])
        d2(i, up, 1, 3, 5, down).start()

    def gather_end(i):
        got(tile_part(i, down, 1), d2_recv.at[i, 1])
        got(tile_part(i, up, 0), d2_recv.at[i, 3])
        got(tile_part(i, z_far, 0), d2_recv.at[i, 4])
        got(tile_part(i, z_far, 1), d2_recv.at[i, 5])

    y_mine = y_all.at[:, pl.ds(pl.multiple_of(zi * cols, 128), cols)]

    def project(i):
        lhs = jnp.concatenate([og[i, s] for s in range(tp_size)], axis=1)
        y_send[i] = jnp.dot(lhs, w_buf[...], preferred_element_type=jnp.float32).astype(jnp.bfloat16)

    half = chunk // 2

    def y_part(h, z):
        return y_all.at[pl.ds(h * half, half), pl.ds(pl.multiple_of(z * cols, 128), cols)]

    def deliver(i):
        dist = lax.rem(i - zi + side, side)

        @pl.when(lax.rem(dist, 2) == 1)
        def _():
            move(y_send.at[i], y_mine, d3_send.at[0], d3_recv.at[0], "tp", i * side + yi).start()

        @pl.when(dist == 2)
        def _():
            move(y_send.at[i, pl.ds(0, half)], relay.at[0], d3_send.at[1], relay_recv.at[0], "tp", up * side + yi).start()
            move(y_send.at[i, pl.ds(half, half)], relay.at[1], d3_send.at[1], relay_recv.at[1], "tp", down * side + yi).start()

        @pl.when(dist == 0)
        def _():
            y_all[:, pl.ds(pl.multiple_of(zi * cols, 128), cols)] = y_send[i]

    def hand_on(i):
        dist = lax.rem(i - zi + side, side)

        @pl.when(dist == 1)
        def _():
            got(relay.at[0], relay_recv.at[0])
            move(relay.at[0], y_part(0, down), d3_send.at[2], d3_recv.at[1], "tp", up * side + yi).start()

        @pl.when(dist == 3)
        def _():
            got(relay.at[1], relay_recv.at[1])
            move(relay.at[1], y_part(1, up), d3_send.at[3], d3_recv.at[2], "tp", down * side + yi).start()

    def tile(i, _):
        is_low = i < 2
        count = jnp.where(is_low, cp, 2 * cp_size - 1 - cp)
        before = jnp.where(is_low, i * cp, 2 * cp + (i - 2) * (2 * cp_size - 1 - cp))

        @pl.when(lax.rem(i, 2) == 0)
        def _():
            diag(i, 0)

        @pl.when(lax.rem(i, 2) == 1)
        def _():
            diag(i, 1)

        @pl.when(i == 0)
        def _():
            kv_forward(tp_size - 1)
            kv_far(tp_size - 2)
            kv_far(tp_size - 1)
            for k in range(4):
                got(kv.at[pl.ds(0, block)], pair_recv.at[k])

        def piece_base(j):
            return jnp.where(j < cp_size, j * 2 * piece, (2 * cp_size - 1 - j) * 2 * piece + piece)

        def look(g, base):
            ahead_sc = scores(i, g, base, piece)
            s_ref[g][...] = ahead_sc
            return ahead_sc

        def full(j, _):
            base = piece_base(j)
            later = piece_base(jnp.minimum(j + 1, count - 1))
            turn = before + j
            services = [(at, functools.partial(w_share, grp)) for grp, at in enumerate((0, 1, 3, 7))]
            services += [(at, functools.partial(w_pass, grp)) for grp, at in enumerate((9, 14, 19, 24))]
            services += [(at, functools.partial(w_last, grp)) for grp, at in enumerate((27, 29))]
            services += [(low_turn, start_low), (low_turn + 9, pass_low)]
            services += [(high_turn, functools.partial(gather_start, 2)), (high_turn + 4, functools.partial(gather_pass, 2))]
            due = functools.reduce(jnp.add, [jnp.where(turn == at, 1, 0) for at, _ in services])

            def serve(_, carry):
                for at, act in services:
                    pl.when(turn == at)(act)
                return carry

            lax.fori_loop(0, jnp.minimum(due, 1), serve, 0)

            for g in range(group):
                top = jnp.max(x_ref[g], axis=0, keepdims=True) * coef
                m_old = m_ref[g, 0:1, :]
                m_new = jnp.maximum(m_old, top)
                scale = jnp.exp2(m_old - m_new)
                m_ref[g, 0:1, :] = m_new
                total = l_ref[g] * scale
                nxt = look((g + 1) % group, base if g + 1 < group else later)
                p = jnp.exp2(s_ref[g][...] * coef - m_new)
                total = total + fold(p, jnp.add)
                p = p.astype(jnp.bfloat16)
                peak = fold(nxt, jnp.maximum)
                acc_ref[g] = acc_ref[g] * scale + values(p, base, piece)
                l_ref[g] = total
                x_ref[(g + 1) % group] = peak
            return 0

        @pl.when(count > 0)
        def _():
            x_ref[0] = fold(look(0, piece_base(0)), jnp.maximum)

        lax.fori_loop(0, count, full, 0)
        for g in range(group):
            total = jnp.sum(l_ref[g], axis=0, keepdims=True)
            out = (acc_ref[g] / total).T.astype(jnp.bfloat16)
            for k in range(side):
                o_buf[i, k, :, g * HEAD_DIM:(g + 1) * HEAD_DIM] = out[k * chunk:(k + 1) * chunk]
        og[i, tp] = o_buf[i, yi]
        for k in range(1, side):
            d1(i, k).start()
        return 0

    def start_low():
        gather_start(0)
        gather_start(1)

    def pass_low():
        gather_pass(0)
        gather_pass(1)

    low_turn = jnp.maximum(2 * cp + 2, 12)
    high_turn = cp + 2 * cp_size + 2
    s_ref = (s_even, s_odd)
    lax.fori_loop(0, side, tile, 0)

    gather_start(3)
    w_last(2)
    w_last(3)
    for k in range(16, 20):
        got(w_part, w_recv.at[k])
    for i in range(3):
        gather_end(i)
    project(0)
    gather_pass(3)
    lax.fori_loop(1, 3, lambda i, c: (project(i), c)[1], 0)
    for i in range(3):
        deliver(i)
    gather_end(3)
    project(3)
    deliver(3)
    for i in range(4):
        hand_on(i)
    got(y_all.at[:, pl.ds(0, 2 * cols)], d3_recv.at[0])
    got(relay.at[0], d3_recv.at[1])
    got(relay.at[1], d3_recv.at[2])
    out = pltpu.make_async_copy(y_all, y_hbm, load_sem.at[0])
    out.start()
    for s in range(4):
        sent(xg.at[pl.ds(0, (tp_size - 1) * part)], ring_send.at[s])
    for k in range(7):
        sent(kv.at[pl.ds(0, block)], kv_send.at[k])
    sent(w_buf.at[pl.ds(0, (tp_size - 1) * slab)], w_send.at[0])
    for k in range(1, 8):
        sent(w_part, w_send.at[k])
    sent(o_buf.at[:, pl.ds(0, side - 1)], d1_send.at[0])
    sent(og.at[:, pl.ds(0, side)], d2_send.at[0])
    sent(og.at[:, pl.ds(0, side)], d2_send.at[1])
    sent(og.at[:, pl.ds(0, side), pl.ds(0, chunk // 2)], d2_send.at[2])
    sent(og.at[:, pl.ds(0, side), pl.ds(0, chunk // 2)], d2_send.at[3])
    sent(y_send.at[pl.ds(0, 2)], d3_send.at[0])
    sent(y_send.at[0], d3_send.at[1])
    sent(relay.at[0], d3_send.at[2])
    sent(relay.at[1], d3_send.at[3])
    out.wait()


def layer(tp_size, cp_size, x_loc, w_q, w_k, w_v, w_o):
    rows, depth = x_loc.shape
    block = rows * tp_size
    q_width = w_q.shape[1]
    kv_width = w_k.shape[1] + w_v.shape[1]
    group = q_width // HEAD_DIM
    model_width = w_o.shape[1]
    side = 4
    cols = model_width // side
    any_space = pl.BlockSpec(memory_space=pl.ANY)
    dma = pltpu.SemaphoreType.DMA
    bf16 = jnp.bfloat16
    flops = 2 * block * depth * (2 * q_width + kv_width) + 2 * block * q_width * block * cp_size
    return pl.pallas_call(
        functools.partial(layer_kernel, tp_size, cp_size),
        out_shape=jax.ShapeDtypeStruct((rows, model_width), bf16),
        in_specs=[any_space] * 5,
        out_specs=any_space,
        scratch_shapes=[
            pltpu.VMEM((block, depth), bf16),
            pltpu.VMEM((depth, q_width + kv_width), bf16),
            pltpu.VMEM((block, q_width), bf16),
            pltpu.VMEM((block * cp_size, kv_width), bf16),
            pltpu.VMEM((w_o.shape[0] * tp_size, cols), bf16),
            pltpu.VMEM((w_o.shape[0] // cp_size, model_width), bf16),
            pltpu.VMEM((side, tp_size, rows, q_width), bf16),
            pltpu.VMEM((side, side, rows, q_width), bf16),
            pltpu.VMEM((side, rows, cols), bf16),
            pltpu.VMEM((rows, model_width), bf16),
            pltpu.VMEM((2, rows // 2, cols), bf16),
        ] + [pltpu.VMEM((group, HEAD_DIM, SUB), jnp.float32)] + [pltpu.VMEM((group, 8, SUB), jnp.float32) for _ in range(3)] + [pltpu.VMEM((block // 2, SUB), jnp.float32) for _ in range(2)] + [
            dma((6,)), dma((4,)), dma((4, tp_size - 1, X_SUB)), dma((7,)), dma((tp_size,)), dma((tp_size,)), dma((tp_size,)), dma((4,)),
            dma((8,)), dma((20,)), dma((1,)), dma((side,)), dma((4,)), dma((side, 6)), dma((4,)), dma((3,)), dma((2,)),
        ],
        compiler_params=pltpu.CompilerParams(collective_id=0, has_side_effects=True, vmem_limit_bytes=67043328),
        cost_estimate=pl.CostEstimate(flops=flops, bytes_accessed=block * depth * 2, transcendentals=0),
        name="layer",
    )(x_loc, w_q, w_k, w_v, w_o)


def solution(mesh):
    cp_size = mesh.shape["cp"]
    tp_size = mesh.shape["tp"]
    row_spec = P(("dp", "cp", "tp"), None)
    local_layer = functools.partial(layer, tp_size, cp_size)
    return jax.shard_map(local_layer, mesh=mesh, in_specs=(row_spec, P(None, "tp"), P(None, "tp"), P(None, "tp"), P("tp", None)), out_specs=row_spec, check_vma=False)
```

```python
import functools

import jax
import jax.numpy as jnp
from jax import lax
from jax.experimental import pallas as pl
from jax.experimental.pallas import tpu as pltpu
from jax.sharding import PartitionSpec as P

HEAD_DIM = 128
LOG2E = 1.4426950408889634
NT = (((1,), (1,)), ((), ()))
SUB = 512


MESH = pl.DeviceIdType.MESH
X_SUB = 2


def layer_kernel(tp_size, cp_size, x_hbm, wq_hbm, wk_hbm, wv_hbm, wo_hbm, y_hbm, xg, w_in, q_buf, kv, w_buf, wo_buf, og, o_buf, y_send, y_all, relay, acc_ref, m_ref, l_ref, x_ref, s_even, s_odd, load_sem, ring_send, ring_recv, kv_send, left_recv, right_recv, far_recv, pair_recv, w_send, w_recv, d1_send, d1_recv, d2_send, d2_recv, d3_send, d3_recv, relay_recv):
    tp = lax.axis_index("tp")
    cp = lax.axis_index("cp")
    side = 4
    zi, yi = tp // side, lax.rem(tp, side)
    chip, core = cp // 2, lax.rem(cp, 2)
    n_chip = cp_size // 2
    rows = x_hbm.shape[0]
    piece = q_buf.shape[0] // 2
    group = q_buf.shape[1] // HEAD_DIM
    chunk = SUB // side
    slab = wo_buf.shape[0]
    head_rows = slab * cp_size
    cols = w_buf.shape[1]
    coef = LOG2E * HEAD_DIM ** -0.5
    up = lax.rem(zi + 1, side)
    down = lax.rem(zi + side - 1, side)
    z_far = lax.rem(zi + 2, side)
    block = rows * tp_size
    part = rows // 4
    sub = part // X_SUB
    q_width = wq_hbm.shape[1]
    k_width = wk_hbm.shape[1]
    pos = (zi * side + lax.rem(yi + zi, side), yi * side + lax.rem(zi + yi, side))

    def member(cycle, k):
        k = lax.rem(k + 2 * tp_size, tp_size)
        major = k // side
        minor = lax.rem(k - major + side, side)
        return major * side + minor if cycle == 0 else minor * side + major

    streams = [(0, 1), (0, -1), (1, 1), (1, -1)]
    nxt = [member(c, pos[c] + d) for c, d in streams]
    right = lax.rem(chip + 1, n_chip) * 2 + core
    left = lax.rem(chip + n_chip - 1, n_chip) * 2 + core
    far = lax.rem(chip + 2, n_chip) * 2 + core
    pair = cp + 1 - 2 * core
    ahead = jnp.where(core == 0, right, left)
    behind = jnp.where(core == 0, left, right)

    w_q = pltpu.make_async_copy(wq_hbm, w_in.at[:, pl.ds(0, q_width)], load_sem.at[0])
    w_k = pltpu.make_async_copy(wk_hbm, w_in.at[:, pl.ds(q_width, k_width)], load_sem.at[1])
    w_v = pltpu.make_async_copy(wv_hbm, w_in.at[:, pl.ds(q_width + k_width, k_width)], load_sem.at[2])
    own = pltpu.make_async_copy(x_hbm, xg.at[pl.ds(pl.multiple_of(tp * rows, rows), rows)], load_sem.at[3])
    load_w = pltpu.make_async_copy(wo_hbm.at[pl.ds(pl.multiple_of(cp * slab, slab), slab)], wo_buf, load_sem.at[4])
    own.start()
    w_q.start()
    w_k.start()
    w_v.start()
    load_w.start()

    barrier = pltpu.get_barrier_semaphore()
    for k in range(1, tp_size):
        pl.semaphore_signal(barrier, inc=1, device_id={"tp": lax.rem(tp + k, tp_size)}, device_id_type=MESH)
    for peer in (left, right, pair):
        pl.semaphore_signal(barrier, inc=1, device_id={"cp": peer}, device_id_type=MESH)
    pl.semaphore_wait(barrier, tp_size + 2)
    own.wait()

    def source(s, t):
        c, d = streams[s]
        return member(c, pos[c] - d * t)

    def move(src, dst, send_sem, recv_sem, axis, peer):
        return pltpu.make_async_remote_copy(src_ref=src, dst_ref=dst, send_sem=send_sem, recv_sem=recv_sem, device_id={axis: peer}, device_id_type=MESH)

    def kv_rows(owner, s, t):
        return kv.at[pl.ds(pl.multiple_of(owner * block + source(s, t) * rows + s * part, part), part)]

    def got(ref, recv_sem):
        move(ref, ref, w_send.at[0], recv_sem, "cp", pair).wait_recv()

    def sent(ref, send_sem):
        move(ref, ref, send_sem, w_recv.at[0], "cp", pair).wait_send()

    kv_unit = kv.at[pl.ds(0, rows)]

    def kv_own(u):
        for s in range(4):
            at = kv_rows(cp, s, u)
            move(at, at, kv_send.at[0], left_recv.at[u], "cp", right).start()
            move(at, at, kv_send.at[1], right_recv.at[u], "cp", left).start()
            move(at, at, kv_send.at[2], pair_recv.at[0], "cp", pair).start()

    def kv_forward(u):
        got(kv_unit, left_recv.at[u])
        got(kv_unit, right_recv.at[u])
        for s in range(4):
            at = kv_rows(behind, s, u)
            move(at, at, kv_send.at[3], far_recv.at[u], "cp", ahead).start()
            at = kv_rows(left, s, u)
            move(at, at, kv_send.at[4], pair_recv.at[1], "cp", pair).start()
            at = kv_rows(right, s, u)
            move(at, at, kv_send.at[5], pair_recv.at[2], "cp", pair).start()

    def kv_far(u):
        got(kv_unit, far_recv.at[u])
        for s in range(4):
            at = kv_rows(far, s, u)
            move(at, at, kv_send.at[6], pair_recv.at[3], "cp", pair).start()

    def w_rows(owner, member):
        return w_buf.at[pl.ds(pl.multiple_of(owner * head_rows + member * slab, slab), slab)]

    def w_cols(quarter):
        return wo_buf.at[:, pl.ds(pl.multiple_of(quarter * cols, 128), cols)]

    own_w = pltpu.make_async_copy(w_cols(zi), w_rows(tp, cp), load_sem.at[5])

    n_group = 4
    per_group = tp_size // n_group

    def w_fetch():
        for k in range(1, tp_size):
            peer = lax.rem(tp + k, tp_size)
            move(w_cols(peer // side), w_rows(tp, cp), w_send.at[0], w_recv.at[k // per_group], "tp", peer).start()

    def w_sources(grp):
        return [lax.rem(tp - k + tp_size, tp_size) for k in range(grp * per_group, (grp + 1) * per_group)]

    w_group = w_buf.at[pl.ds(0, per_group * slab)]

    def step(t, _):
        @pl.when(t == tp_size - 1)
        def _():
            load_w.wait()
            own_w.start()
            w_fetch()

        for u in range(X_SUB):
            for s in range(4):
                at = xg.at[pl.ds(pl.multiple_of(source(s, t) * rows + s * part + u * sub, sub), sub)]

                @pl.when(t > 0)
                def _():
                    move(at, at, ring_send.at[s], ring_recv.at[s, t - 1, u], "tp", nxt[s]).wait_recv()

                @pl.when(t < tp_size - 1)
                def _():
                    move(at, at, ring_send.at[s], ring_recv.at[s, t, u], "tp", nxt[s]).start()

        @pl.when(t >= 1)
        def _():
            kv_own(t - 1)

        @pl.when(t >= 2)
        def _():
            kv_forward(t - 2)

        @pl.when(t >= 3)
        def _():
            kv_far(t - 3)

        @pl.when(t == 0)
        def _():
            w_q.wait()
            w_k.wait()
            w_v.wait()

        offs = [pl.multiple_of(source(s, t) * rows + s * part, part) for s in range(4)]
        lhs = jnp.concatenate([xg[pl.ds(o, part), :] for o in offs], axis=0)
        res = jnp.dot(lhs, w_in[...], preferred_element_type=jnp.float32).astype(jnp.bfloat16)
        for s in range(4):
            q_buf[pl.ds(offs[s], part), :] = res[s * part:(s + 1) * part, 0:q_width]
            kv[pl.ds(pl.multiple_of(cp * block + offs[s], part), part), :] = res[s * part:(s + 1) * part, q_width:]
        return 0

    lax.fori_loop(0, tp_size, step, 0)
    kv_own(tp_size - 1)
    kv_forward(tp_size - 2)
    kv_far(tp_size - 3)

    def w_share(grp):
        if grp == 0:
            own_w.wait()
            got(w_buf.at[pl.ds(0, (per_group - 1) * slab)], w_recv.at[0])
        else:
            got(w_group, w_recv.at[grp])
        for o in w_sources(grp):
            ref = w_rows(o, cp)
            move(ref, ref, w_send.at[1], w_recv.at[4 + grp], "cp", right).start()
            move(ref, ref, w_send.at[2], w_recv.at[8 + grp], "cp", left).start()
            move(ref, ref, w_send.at[3], w_recv.at[16], "cp", pair).start()

    def w_pass(grp):
        got(w_group, w_recv.at[4 + grp])
        got(w_group, w_recv.at[8 + grp])
        for o in w_sources(grp):
            ref = w_rows(o, behind)
            move(ref, ref, w_send.at[4], w_recv.at[12 + grp], "cp", ahead).start()
            ref = w_rows(o, left)
            move(ref, ref, w_send.at[5], w_recv.at[17], "cp", pair).start()
            ref = w_rows(o, right)
            move(ref, ref, w_send.at[6], w_recv.at[18], "cp", pair).start()

    def w_last(grp):
        got(w_group, w_recv.at[12 + grp])
        for o in w_sources(grp):
            ref = w_rows(o, far)
            move(ref, ref, w_send.at[7], w_recv.at[19], "cp", pair).start()

    w_part = w_buf.at[pl.ds(0, tp_size * slab)]

    def fold(x, op):
        total = x[0:8]
        for c in range(1, x.shape[0] // 8):
            total = op(total, x[c * 8:(c + 1) * 8])
        return total

    def scores(i, g, base, width):
        qs = q_buf[pl.ds(pl.multiple_of(i * SUB, SUB), SUB), g * HEAD_DIM:(g + 1) * HEAD_DIM]
        ks = kv[pl.ds(pl.multiple_of(base, SUB), width), 0:HEAD_DIM]
        return lax.dot_general(ks, qs, NT, preferred_element_type=jnp.float32)

    def values(p, base, width):
        vs = kv[pl.ds(pl.multiple_of(base, SUB), width), HEAD_DIM:2 * HEAD_DIM]
        return jnp.dot(vs.T, p, preferred_element_type=jnp.float32)

    def diag(i, s):
        width = (s + 1) * SUB
        base = cp * 2 * piece + (i // 2) * piece
        for g in range(group):
            sc = scores(i, g, base, width)
            key = lax.broadcasted_iota(jnp.int32, (width, SUB), 0)
            query = lax.broadcasted_iota(jnp.int32, (width, SUB), 1) + s * SUB
            sc = jnp.where(query >= key, sc, -jnp.inf)
            top = jnp.max(sc, axis=0, keepdims=True) * coef
            p = jnp.exp2(sc * coef - top)
            m_ref[g, 0:1, :] = top
            l_ref[g] = fold(p, jnp.add)
            acc_ref[g] = values(p.astype(jnp.bfloat16), base, width)

    def d1(i, k):
        peer = lax.rem(yi + k, side)
        return move(o_buf.at[i, peer], og.at[i, tp], d1_send.at[0], d1_recv.at[i], "tp", zi * side + peer)

    def tile_part(i, z, half):
        return og.at[i, pl.ds(z * side, side), pl.ds(half * (chunk // 2), chunk // 2)]

    def d2(i, z, half, send, recv, peer):
        ref = tile_part(i, z, half)
        return move(ref, ref, d2_send.at[send], d2_recv.at[i, recv], "tp", peer * side + yi)

    def gather_start(i):
        got(og.at[i, pl.ds(0, side - 1)], d1_recv.at[i])
        d2(i, zi, 0, 0, 0, up).start()
        d2(i, zi, 1, 1, 2, down).start()
        d2(i, zi, 1, 0, 1, up).start()
        d2(i, zi, 0, 1, 3, down).start()

    def gather_pass(i):
        got(tile_part(i, down, 0), d2_recv.at[i, 0])
        d2(i, down, 0, 2, 4, up).start()
        got(tile_part(i, up, 1), d2_recv.at[i, 2])
        d2(i, up, 1, 3, 5, down).start()

    def gather_end(i):
        got(tile_part(i, down, 1), d2_recv.at[i, 1])
        got(tile_part(i, up, 0), d2_recv.at[i, 3])
        got(tile_part(i, z_far, 0), d2_recv.at[i, 4])
        got(tile_part(i, z_far, 1), d2_recv.at[i, 5])

    y_mine = y_all.at[:, pl.ds(pl.multiple_of(zi * cols, 128), cols)]

    def project(i):
        lhs = jnp.concatenate([og[i, s] for s in range(tp_size)], axis=1)
        y_send[i] = jnp.dot(lhs, w_buf[...], preferred_element_type=jnp.float32).astype(jnp.bfloat16)

    half = chunk // 2

    def y_part(h, z):
        return y_all.at[pl.ds(h * half, half), pl.ds(pl.multiple_of(z * cols, 128), cols)]

    def deliver(i):
        dist = lax.rem(i - zi + side, side)

        @pl.when(lax.rem(dist, 2) == 1)
        def _():
            move(y_send.at[i], y_mine, d3_send.at[0], d3_recv.at[0], "tp", i * side + yi).start()

        @pl.when(dist == 2)
        def _():
            move(y_send.at[i, pl.ds(0, half)], relay.at[0], d3_send.at[1], relay_recv.at[0], "tp", up * side + yi).start()
            move(y_send.at[i, pl.ds(half, half)], relay.at[1], d3_send.at[1], relay_recv.at[1], "tp", down * side + yi).start()

        @pl.when(dist == 0)
        def _():
            y_all[:, pl.ds(pl.multiple_of(zi * cols, 128), cols)] = y_send[i]

    def hand_on(i):
        dist = lax.rem(i - zi + side, side)

        @pl.when(dist == 1)
        def _():
            got(relay.at[0], relay_recv.at[0])
            move(relay.at[0], y_part(0, down), d3_send.at[2], d3_recv.at[1], "tp", up * side + yi).start()

        @pl.when(dist == 3)
        def _():
            got(relay.at[1], relay_recv.at[1])
            move(relay.at[1], y_part(1, up), d3_send.at[3], d3_recv.at[2], "tp", down * side + yi).start()

    def tile(i, _):
        is_low = i < 2
        count = jnp.where(is_low, cp, 2 * cp_size - 1 - cp)
        before = jnp.where(is_low, i * cp, 2 * cp + (i - 2) * (2 * cp_size - 1 - cp))

        @pl.when(lax.rem(i, 2) == 0)
        def _():
            diag(i, 0)

        @pl.when(lax.rem(i, 2) == 1)
        def _():
            diag(i, 1)

        @pl.when(i == 0)
        def _():
            kv_forward(tp_size - 1)
            kv_far(tp_size - 2)
            kv_far(tp_size - 1)
            for k in range(4):
                got(kv.at[pl.ds(0, block)], pair_recv.at[k])

        def piece_base(j):
            return jnp.where(j < cp_size, j * 2 * piece, (2 * cp_size - 1 - j) * 2 * piece + piece)

        def look(g, base):
            ahead_sc = scores(i, g, base, piece)
            s_ref[g][...] = ahead_sc
            return ahead_sc

        def full(j, _):
            base = piece_base(j)
            later = piece_base(jnp.minimum(j + 1, count - 1))
            turn = before + j
            services = [(at, functools.partial(w_share, grp)) for grp, at in enumerate((0, 2, 5, 10))]
            services += [(at, functools.partial(w_pass, grp)) for grp, at in enumerate((11, 17, 23, 28))]
            services += [(at, functools.partial(w_last, grp)) for grp, at in enumerate((27, 29))]
            services += [(low_turn, start_low), (low_turn + 11, pass_low)]
            services += [(high_turn, functools.partial(gather_start, 2)), (high_turn + 4, functools.partial(gather_pass, 2))]
            due = functools.reduce(jnp.add, [jnp.where(turn == at, 1, 0) for at, _ in services])

            def serve(_, carry):
                for at, act in services:
                    pl.when(turn == at)(act)
                return carry

            lax.fori_loop(0, jnp.minimum(due, 1), serve, 0)

            for g in range(group):
                top = jnp.max(x_ref[g], axis=0, keepdims=True) * coef
                m_old = m_ref[g, 0:1, :]
                m_new = jnp.maximum(m_old, top)
                scale = jnp.exp2(m_old - m_new)
                m_ref[g, 0:1, :] = m_new
                total = l_ref[g] * scale
                nxt = look((g + 1) % group, base if g + 1 < group else later)
                p = jnp.exp2(s_ref[g][...] * coef - m_new)
                total = total + fold(p, jnp.add)
                p = p.astype(jnp.bfloat16)
                peak = fold(nxt, jnp.maximum)
                acc_ref[g] = acc_ref[g] * scale + values(p, base, piece)
                l_ref[g] = total
                x_ref[(g + 1) % group] = peak
            return 0

        @pl.when(count > 0)
        def _():
            x_ref[0] = fold(look(0, piece_base(0)), jnp.maximum)

        lax.fori_loop(0, count, full, 0)
        for g in range(group):
            total = jnp.sum(l_ref[g], axis=0, keepdims=True)
            out = (acc_ref[g] / total).T.astype(jnp.bfloat16)
            for k in range(side):
                o_buf[i, k, :, g * HEAD_DIM:(g + 1) * HEAD_DIM] = out[k * chunk:(k + 1) * chunk]
        og[i, tp] = o_buf[i, yi]
        for k in range(1, side):
            d1(i, k).start()
        return 0

    def start_low():
        gather_start(0)
        gather_start(1)

    def pass_low():
        gather_pass(0)
        gather_pass(1)

    low_turn = jnp.maximum(2 * cp + 2, 12)
    high_turn = cp + 2 * cp_size + 2
    s_ref = (s_even, s_odd)
    lax.fori_loop(0, side, tile, 0)

    gather_start(3)
    w_last(2)
    w_last(3)
    for k in range(16, 20):
        got(w_part, w_recv.at[k])
    for i in range(3):
        gather_end(i)
    project(0)
    gather_pass(3)
    lax.fori_loop(1, 3, lambda i, c: (project(i), c)[1], 0)
    for i in range(3):
        deliver(i)
    gather_end(3)
    project(3)
    deliver(3)
    for i in range(4):
        hand_on(i)
    got(y_all.at[:, pl.ds(0, 2 * cols)], d3_recv.at[0])
    got(relay.at[0], d3_recv.at[1])
    got(relay.at[1], d3_recv.at[2])
    out = pltpu.make_async_copy(y_all, y_hbm, load_sem.at[0])
    out.start()
    for s in range(4):
        sent(xg.at[pl.ds(0, (tp_size - 1) * part)], ring_send.at[s])
    for k in range(7):
        sent(kv.at[pl.ds(0, block)], kv_send.at[k])
    sent(w_buf.at[pl.ds(0, (tp_size - 1) * slab)], w_send.at[0])
    for k in range(1, 8):
        sent(w_part, w_send.at[k])
    sent(o_buf.at[:, pl.ds(0, side - 1)], d1_send.at[0])
    sent(og.at[:, pl.ds(0, side)], d2_send.at[0])
    sent(og.at[:, pl.ds(0, side)], d2_send.at[1])
    sent(og.at[:, pl.ds(0, side), pl.ds(0, chunk // 2)], d2_send.at[2])
    sent(og.at[:, pl.ds(0, side), pl.ds(0, chunk // 2)], d2_send.at[3])
    sent(y_send.at[pl.ds(0, 2)], d3_send.at[0])
    sent(y_send.at[0], d3_send.at[1])
    sent(relay.at[0], d3_send.at[2])
    sent(relay.at[1], d3_send.at[3])
    out.wait()


def layer(tp_size, cp_size, x_loc, w_q, w_k, w_v, w_o):
    rows, depth = x_loc.shape
    block = rows * tp_size
    q_width = w_q.shape[1]
    kv_width = w_k.shape[1] + w_v.shape[1]
    group = q_width // HEAD_DIM
    model_width = w_o.shape[1]
    side = 4
    cols = model_width // side
    any_space = pl.BlockSpec(memory_space=pl.ANY)
    dma = pltpu.SemaphoreType.DMA
    bf16 = jnp.bfloat16
    flops = 2 * block * depth * (2 * q_width + kv_width) + 2 * block * q_width * block * cp_size
    return pl.pallas_call(
        functools.partial(layer_kernel, tp_size, cp_size),
        out_shape=jax.ShapeDtypeStruct((rows, model_width), bf16),
        in_specs=[any_space] * 5,
        out_specs=any_space,
        scratch_shapes=[
            pltpu.VMEM((block, depth), bf16),
            pltpu.VMEM((depth, q_width + kv_width), bf16),
            pltpu.VMEM((block, q_width), bf16),
            pltpu.VMEM((block * cp_size, kv_width), bf16),
            pltpu.VMEM((w_o.shape[0] * tp_size, cols), bf16),
            pltpu.VMEM((w_o.shape[0] // cp_size, model_width), bf16),
            pltpu.VMEM((side, tp_size, rows, q_width), bf16),
            pltpu.VMEM((side, side, rows, q_width), bf16),
            pltpu.VMEM((side, rows, cols), bf16),
            pltpu.VMEM((rows, model_width), bf16),
            pltpu.VMEM((2, rows // 2, cols), bf16),
        ] + [pltpu.VMEM((group, HEAD_DIM, SUB), jnp.float32)] + [pltpu.VMEM((group, 8, SUB), jnp.float32) for _ in range(3)] + [pltpu.VMEM((block // 2, SUB), jnp.float32) for _ in range(2)] + [
            dma((6,)), dma((4,)), dma((4, tp_size - 1, X_SUB)), dma((7,)), dma((tp_size,)), dma((tp_size,)), dma((tp_size,)), dma((4,)),
            dma((8,)), dma((20,)), dma((1,)), dma((side,)), dma((4,)), dma((side, 6)), dma((4,)), dma((3,)), dma((2,)),
        ],
        compiler_params=pltpu.CompilerParams(collective_id=0, has_side_effects=True, vmem_limit_bytes=67043328),
        cost_estimate=pl.CostEstimate(flops=flops, bytes_accessed=block * depth * 2, transcendentals=0),
        name="layer",
    )(x_loc, w_q, w_k, w_v, w_o)


def solution(mesh):
    cp_size = mesh.shape["cp"]
    tp_size = mesh.shape["tp"]
    row_spec = P(("dp", "cp", "tp"), None)
    local_layer = functools.partial(layer, tp_size, cp_size)
    return jax.shard_map(local_layer, mesh=mesh, in_specs=(row_spec, P(None, "tp"), P(None, "tp"), P(None, "tp"), P("tp", None)), out_specs=row_spec, check_vma=False)
```
